512 devices in a mesh: gz: 8 (over x, y_lo), xy: 64 (over z, y_hi, core).
Axes of the slice: x: 4, y: 4 (y_hi: 2, y_lo: 2; y = y_hi * 2 + y_lo), z: 16, core: 2. Of those that a mesh axis runs over, the one named last changes fastest.
Arguments:
- fixed: float32 [64, 1024, 1024], P('gz', 'xy'), may hold values from -6 to 6
- moving: float32 [64, 1024, 1024], P('gz', 'xy'), may hold values from -9 to 9
Outputs:
- update: float32 [3, 64, 1024, 1024], P(None, 'gz', 'xy')
The draws below stay inside these ranges and needn't reach their ends.
All inputs are finite; a program needn't handle non-finite values.
Results may differ from the reference program's by a relative error of at most 0.00016.
Values sent between devices are 32-bit elements; how exact they have to be, the bound alone decides.
No kernel may reach another device: no remote copies, remote signals or barrier semaphores. Data moves between devices by JAX's collectives and lax.ppermute only.
A program may use at most 64 MiB of HBM per device.

```python
import jax
import jax.numpy as jnp
from jax import lax

RADIUS = 4
SPACING = 8
NX = 1024
NZ = 64
NY = 1024


def image_pair(key):
    first_key, second_key = jax.random.split(jax.random.fold_in(key, 7))
    shape = (NZ, NY, NX)
    base = jnp.clip(jax.random.normal(first_key, shape, jnp.float32), -6.0, 6.0)
    noise = jnp.clip(jax.random.normal(second_key, shape, jnp.float32), -6.0, 6.0)
    lower, upper = (0.1, 0.8)
    plane = jnp.arange(NZ).astype(jnp.float32) / NZ
    row = jnp.arange(NY).astype(jnp.float32) / NY
    weight = lower + (upper - lower) * 0.5 * (plane[:, None, None] + row[None, :, None])
    moved = weight * base + jnp.sqrt(1.0 - weight * weight) * noise
    return (base, moved)


def draw_fixed(key, part):
    return image_pair(key)[0].astype(jnp.float32)


def draw_moving(key, part):
    return image_pair(key)[1].astype(jnp.float32)


def setup_inputs(seed: int = 0) -> dict:
    arg_keys = jax.random.split(jax.random.key(seed), 3)
    return {
        "fixed": draw_fixed(jax.random.fold_in(arg_keys[2], 71), 0),
        "moving": draw_moving(jax.random.fold_in(arg_keys[2], 71), 0),
    }


HIGH = lax.Precision.HIGHEST
EPS = 1e-05

def basis(index, knot):
    span = index // SPACING
    frac = (index - span * SPACING).astype(jnp.float32) / SPACING
    offset = knot - span
    other = 1.0 - frac
    first = other * other * other / 6.0
    second = (3.0 * frac ** 3 - 6.0 * frac ** 2 + 4.0) / 6.0
    third = (-3.0 * frac ** 3 + 3.0 * frac ** 2 + 3.0 * frac + 1.0) / 6.0
    fourth = frac ** 3 / 6.0
    zero = jnp.zeros_like(frac)
    return jnp.where(offset == 0, first, jnp.where(offset == 1, second, jnp.where(offset == 2, third, jnp.where(offset == 3, fourth, zero))))

def square_total(index):
    span = index // SPACING
    total = basis(index, span) ** 2
    for step in range(1, 4):
        total = total + basis(index, span + step) ** 2
    return total

def fit_matrix(index, knot):
    value = basis(index, knot)
    return value * value * value / square_total(index)

def knot_mass(knot, extent):
    spans = extent // SPACING
    within = jnp.arange(SPACING).astype(jnp.int32)
    offsets = jnp.arange(4).astype(jnp.int32)
    energy = lax.optimization_barrier(jnp.sum(basis(within[None, :], offsets[:, None]) ** 2, axis=1))
    start = knot[:, None] - offsets[None, :]
    valid = (start >= 0) & (start <= spans - 1)
    return lax.optimization_barrier(jnp.sum(jnp.where(valid, energy[None, :], jnp.zeros_like(energy)[None, :]), axis=1))

def window_sum(padded, shape):
    depth, rows, width = shape
    span = 2 * RADIUS + 1
    acc = padded[0:depth]
    for step in range(1, span):
        acc = acc + padded[step:step + depth]
    out = acc[:, 0:rows]
    for step in range(1, span):
        out = out + acc[:, step:step + rows]
    res = out[:, :, 0:width]
    for step in range(1, span):
        res = res + out[:, :, step:step + width]
    return res

def cc_force(fpad, mpad, shape):
    depth, rows, width = shape
    count = float((2 * RADIUS + 1) ** 3)
    sum_f = window_sum(fpad, shape)
    sum_m = window_sum(mpad, shape)
    sum_ff = window_sum(fpad * fpad, shape)
    sum_mm = window_sum(mpad * mpad, shape)
    sum_fm = window_sum(fpad * mpad, shape)
    r = RADIUS
    centre_f = fpad[r:r + depth, r:r + rows, r:r + width]
    centre_m = mpad[r:r + depth, r:r + rows, r:r + width]
    grad_z = (mpad[r + 1:r + 1 + depth, r:r + rows, r:r + width] - mpad[r - 1:r - 1 + depth, r:r + rows, r:r + width]) * 0.5
    grad_y = (mpad[r:r + depth, r + 1:r + 1 + rows, r:r + width] - mpad[r:r + depth, r - 1:r - 1 + rows, r:r + width]) * 0.5
    grad_x = (mpad[r:r + depth, r:r + rows, r + 1:r + 1 + width] - mpad[r:r + depth, r:r + rows, r - 1:r - 1 + width]) * 0.5
    mean_f = sum_f / count
    mean_m = sum_m / count
    cov = sum_fm / count - mean_f * mean_m
    var_f = sum_ff / count - mean_f * mean_f
    var_m = sum_mm / count - mean_m * mean_m
    factor = 2.0 * cov / (var_f * var_m + EPS)
    resid = centre_f - mean_f - cov / (var_m + EPS) * (centre_m - mean_m)
    common = factor * resid
    return jnp.stack([common * grad_z, common * grad_y, common * grad_x])

def reference(fixed, moving):
    depth, rows, width = fixed.shape
    fpad = jnp.pad(fixed, RADIUS)
    mpad = jnp.pad(moving, RADIUS)
    force = cc_force(fpad, mpad, (depth, rows, width))
    knots_z = depth // SPACING + 3
    knots_y = rows // SPACING + 3
    knots_x = width // SPACING + 3
    vox_z = jnp.arange(depth).astype(jnp.int32)
    vox_y = jnp.arange(rows).astype(jnp.int32)
    vox_x = jnp.arange(width).astype(jnp.int32)
    ctl_z = jnp.arange(knots_z).astype(jnp.int32)
    ctl_y = jnp.arange(knots_y).astype(jnp.int32)
    ctl_x = jnp.arange(knots_x).astype(jnp.int32)
    fit_z = fit_matrix(vox_z[None, :], ctl_z[:, None])
    fit_y = fit_matrix(vox_y[None, :], ctl_y[:, None])
    fit_x = fit_matrix(vox_x[None, :], ctl_x[:, None])
    numer = jnp.einsum('kzyx,cx->kzyc', force, fit_x, precision=HIGH)
    numer = jnp.einsum('kzyc,by->kzbc', numer, fit_y, precision=HIGH)
    numer = jnp.einsum('kzbc,az->kabc', numer, fit_z, precision=HIGH)
    mass = knot_mass(ctl_z, depth)[:, None, None] * knot_mass(ctl_y, rows)[None, :, None] * knot_mass(ctl_x, width)[None, None, :]
    coef = numer / mass[None]
    eval_z = basis(vox_z[:, None], ctl_z[None, :])
    eval_y = basis(vox_y[:, None], ctl_y[None, :])
    eval_x = basis(vox_x[:, None], ctl_x[None, :])
    field = jnp.einsum('kabc,xc->kabx', coef, eval_x, precision=HIGH)
    field = jnp.einsum('kabx,yb->kayx', field, eval_y, precision=HIGH)
    field = jnp.einsum('kayx,za->kzyx', field, eval_z, precision=HIGH)
    power = jnp.mean(field * field)
    return field / (jnp.sqrt(power) + 1e-06)
```

```python
import functools

import jax
import jax.numpy as jnp
import numpy as np
from jax import lax
from jax.experimental import pallas as pl
from jax.experimental.pallas import tpu as pltpu
from jax.sharding import Mesh
from jax.sharding import PartitionSpec as P

RADIUS = 4
SPACING = 8
EPS = 1e-05
COUNT = float((2 * RADIUS + 1) ** 3)
XY = ("xy_0", "xy_1", "xy_2")
GZ = ("gz_0", "gz_1")
PLANE = ("gz_0", "gz_1", "xy_1", "xy_2")
SLABS, STRIPS, STACKS = 8, 4, 16
MEMBERS = SLABS * STRIPS
DEPTH, ROWS, WIDTH = 8, 16, 1024
COLS = WIDTH // MEMBERS
WIDE = COLS + 2 * RADIUS
LANES = 128
KZ = SLABS + 3
KY = STRIPS * ROWS // SPACING + 3
F32 = jnp.float32
BF16 = jnp.bfloat16


def np_basis(index, knot):
    span = index // SPACING
    t = (index - span * SPACING) / SPACING
    j = knot - span
    out = np.where(j == 0, (1 - t) ** 3 / 6, 0.0)
    out = np.where(j == 1, (3 * t**3 - 6 * t**2 + 4) / 6, out)
    out = np.where(j == 2, (-3 * t**3 + 3 * t**2 + 3 * t + 1) / 6, out)
    return np.where(j == 3, t**3 / 6, out)


def np_fit(index, knot):
    value = np_basis(index, knot)
    span = index // SPACING
    total = sum(np_basis(index, span + step) ** 2 for step in range(4))
    return value**3 / total


def np_mass(knots, extent):
    spans = extent // SPACING
    within = np.arange(SPACING)
    energy = [np.sum(np_basis(within, np.full(SPACING, j)) ** 2) for j in range(4)]
    return np.array(
        [sum(energy[j] for j in range(4) if 0 <= c - j <= spans - 1) for c in range(knots)]
    )


def tables():
    z8, y16 = np.arange(DEPTH), np.arange(ROWS)
    fit_z = np_fit(z8[None, :], np.arange(4)[:, None])
    fit_y = np_fit(np.arange(STRIPS * ROWS)[None, :], np.arange(16)[:, None])
    fit_zy = np.einsum("az,bqy->abqyz", fit_z, fit_y.reshape(16, STRIPS, ROWS))
    fit_zy[:, KY:] = 0.0
    fit_zy = fit_zy.reshape(64, STRIPS * LANES)
    fit_x = np_fit(np.arange(COLS)[None, :], np.arange(8)[:, None])
    fit_x = np.kron(np.eye(3), fit_x)
    knots_x = WIDTH // SPACING + 3
    mass_x = np_mass(knots_x, WIDTH)
    full_x = np_basis(np.arange(WIDTH)[None, :], np.arange(knots_x)[:, None]) / mass_x[:, None]
    wide_x = np.zeros((MEMBERS, 8, WIDTH))
    for member in range(MEMBERS):
        wide_x[member, :7] = full_x[4 * member : 4 * member + 7]
    wide_x = wide_x.reshape(MEMBERS * 8, WIDTH)
    gram_x = wide_x @ wide_x.T
    eval_z = np_basis(np.arange(SLABS * DEPTH)[:, None], np.arange(KZ)[None, :])
    eval_y = np_basis(np.arange(STRIPS * ROWS)[:, None], np.arange(KY)[None, :])
    gram_zy = np.zeros((LANES, LANES))
    gram_zy[: KZ * KY, : KZ * KY] = np.kron(eval_z.T @ eval_z, eval_y.T @ eval_y)
    mass_z = np_mass(KZ, SLABS * DEPTH)
    mass_y = np_mass(STACKS * 8 + 3, STACKS * STRIPS * ROWS)
    inverse = np.zeros((STACKS, LANES))
    for stack in range(STACKS):
        inverse[stack, : KZ * KY] = (
            1.0 / (mass_z[:, None] * mass_y[None, 8 * stack : 8 * stack + KY])
        ).reshape(-1)
    ez = eval_z.reshape(SLABS, DEPTH, KZ)
    ey = eval_y.reshape(STRIPS, ROWS, KY)
    lane = np.arange(LANES)
    low = np.where((lane < KZ * KY) & (lane % KY < 3), 1.0, 0.0)
    high = np.where((lane < KZ * KY) & (lane % KY >= 8), 1.0, 0.0)
    ez_l = np.zeros((SLABS, DEPTH, LANES))
    ey_l = np.zeros((STRIPS, ROWS, LANES))
    ez_l[..., : KZ * KY] = np.repeat(ez, KY, axis=2)
    ey_l[..., : KZ * KY] = np.tile(ey, (1, 1, KZ))
    f = lambda v: np.asarray(v, np.float32)
    return dict(
        fit_zy=f(fit_zy), fit_x=f(fit_x), wide_x=f(wide_x), gram_x=f(gram_x), gram_zy=f(gram_zy),
        inverse=f(inverse), ez=f(ez_l), ey=f(ey_l), low=f(low), high=f(high),
    )


def split(x):
    hi = x.astype(BF16)
    return hi, (x - hi.astype(F32)).astype(BF16)


def dot(a, b, dims):
    ah, al = split(a)
    bh, bl = split(b)
    d = lambda u, v: lax.dot_general(u, v, (dims, ((), ())), preferred_element_type=F32)
    return d(ah, bh) + d(ah, bl) + d(al, bh)


NN = ((1,), (0,))
NT = ((1,), (1,))


def pack_kernel(f_ref, m_ref, o_ref, s_ref, b_ref):
    zero = jnp.zeros((RADIUS, LANES), F32)
    for image, ref in enumerate((f_ref, m_ref)):
        s_ref[image, 0:RADIUS, :] = zero
        s_ref[image, RADIUS + WIDTH : 2 * RADIUS + WIDTH, :] = zero
        for block in range(WIDTH // LANES):
            buf = b_ref.at[image, block]
            buf[...] = ref[:, block * LANES : (block + 1) * LANES]
            rows = [buf[pl.ds(y, DEPTH, stride=ROWS), :] for y in range(ROWS)]
            tile = jnp.concatenate(rows, axis=0).T
            s_ref[image, RADIUS + block * LANES : RADIUS + (block + 1) * LANES, :] = tile
    for image in range(2):
        for member in range(MEMBERS):
            o_ref[member, image] = s_ref[image, member * COLS : member * COLS + WIDE, :]


def rim_kernel(r_ref, up_ref, down_ref):
    for half in range(2):
        for image in range(2):
            slabs = range(4 * half, 4 * half + 4)
            up_ref[half, image] = jnp.concatenate(
                [r_ref[STRIPS * g + STRIPS - 1, image, :, 96:128] for g in slabs], axis=1
            )
            down_ref[half, image] = jnp.concatenate(
                [r_ref[STRIPS * g, image, :, 0:32] for g in slabs], axis=1
            )


def force_kernel(r_ref, below_ref, above_ref, fz_ref, fx_ref, o_ref, pre, suf, rim, sums, fr, acc, accp):
    lane = lax.broadcasted_iota(jnp.int32, (COLS, LANES), 1)
    z = lane & 7
    y = lane >> 3
    lane_w = lax.broadcasted_iota(jnp.int32, (WIDE, LANES), 1)
    roll = pltpu.roll

    zeros = jnp.zeros((COLS, LANES), F32)
    for q in range(STRIPS + 1):
        for field in range(5):
            suf[0, q, field] = zeros
            pre[SLABS, q, field] = zeros
    for g in range(SLABS):
        for image in range(2):
            b = below_ref[g // 4, image]
            a = above_ref[g // 4, image]
            at = (g % 4) * 32
            b = roll(b, (96 - at) % LANES, 1) if (96 - at) % LANES else b
            a = roll(a, (LANES - at) % LANES, 1) if at else a
            rim[g, image] = jnp.where(lane_w >= 96, b, jnp.where(lane_w < 32, a, 0.0))

    def window_x(v):
        s = v + roll(v, WIDE - 1, 0)
        s = s + roll(s, WIDE - 2, 0)
        s = s + roll(s, WIDE - 4, 0)
        return s[0:COLS] + v[8 : 8 + COLS]

    def images(g, q):
        if q < STRIPS:
            return r_ref[g * STRIPS + q, 0], r_ref[g * STRIPS + q, 1]
        return rim[g, 0], rim[g, 1]

    def phase_a(g, carry):
        for q in range(STRIPS + 1):
            f, m = images(g, q)
            for field, v in enumerate((f, m, f * f, m * m, f * m)):
                w = window_x(v)
                p = w + jnp.where(z >= 1, roll(w, 1, 1), 0.0)
                p = p + jnp.where(z >= 2, roll(p, 2, 1), 0.0)
                p = p + jnp.where(z >= 4, roll(p, 4, 1), 0.0)
                s = w + jnp.where(z < 7, roll(w, LANES - 1, 1), 0.0)
                s = s + jnp.where(z < 6, roll(s, LANES - 2, 1), 0.0)
                s = s + jnp.where(z < 4, roll(s, LANES - 4, 1), 0.0)
                pre[g, q, field] = p
                suf[g + 1, q, field] = s
        return carry

    lax.fori_loop(0, SLABS, phase_a, 0)

    for a in range(KZ):
        acc[a] = jnp.zeros((16, 96), F32)

    def shift_y(d, here, after):
        return roll(jnp.where(y >= d, here, after), LANES - 8 * d, 1)

    def phase_b(g, carry):
        n = STRIPS + 1
        for field in range(5):
            w = []
            for q in range(n):
                t0 = suf[g, q, field] + pre[g, q, field]
                t1 = suf[g + 1, q, field] + pre[g + 1, q, field]
                w.append(jnp.where(z < 4, roll(t0, LANES - 4, 1), roll(t1, 4, 1)))
            s = [w[q] + shift_y(1, w[q], w[(q + 1) % n]) for q in range(n)]
            s = [s[q] + shift_y(2, s[q], s[(q + 1) % n]) for q in range(n)]
            s = [s[q] + shift_y(4, s[q], s[(q + 1) % n]) for q in range(n)]
            t = [s[q] + shift_y(8, w[q], w[(q + 1) % n]) for q in range(n)]
            for q in range(STRIPS):
                sums[field, q] = roll(jnp.where(y < 12, t[q], t[(q - 1) % n]), 32, 1)

        centre = lambda g, q: images(g, q)[1][RADIUS : RADIUS + COLS]
        mid = [centre(g, q) for q in range(n)]
        down = jnp.maximum(g - 1, 0)
        up = jnp.minimum(g + 1, SLABS - 1)
        for q in range(STRIPS):
            f, m = images(g, q)
            fc = f[RADIUS : RADIUS + COLS]
            mc = mid[q]
            grad_x = (m[RADIUS + 1 : RADIUS + 1 + COLS] - m[RADIUS - 1 : RADIUS - 1 + COLS]) * 0.5
            nxt = roll(jnp.where(y >= 1, mc, mid[(q + 1) % n]), LANES - 8, 1)
            prv = roll(jnp.where(y < 15, mc, mid[(q - 1) % n]), 8, 1)
            grad_y = (nxt - prv) * 0.5
            m_up = jnp.where(g < SLABS - 1, centre(up, q), 0.0)
            m_down = jnp.where(g > 0, centre(down, q), 0.0)
            nxt = jnp.where(z < 7, roll(mc, LANES - 1, 1), roll(m_up, 7, 1))
            prv = jnp.where(z > 0, roll(mc, 1, 1), roll(m_down, LANES - 7, 1))
            grad_z = (nxt - prv) * 0.5
            inv = 1.0 / COUNT
            mean_f = sums[0, q] * inv
            mean_m = sums[1, q] * inv
            cov = sums[4, q] * inv - mean_f * mean_m
            var_f = sums[2, q] * inv - mean_f * mean_f
            var_m = sums[3, q] * inv - mean_m * mean_m
            factor = 2.0 * cov / (var_f * var_m + EPS)
            resid = fc - mean_f - cov / (var_m + EPS) * (mc - mean_m)
            common = factor * resid
            at = slice(q * LANES, (q + 1) * LANES)
            fr[0:32, at] = common * grad_z
            fr[32:64, at] = common * grad_y
            fr[64:96, at] = common * grad_x
        part = dot(fz_ref[...], fr[...], NT)
        for a in range(4):
            acc[g + a] += part[16 * a : 16 * a + 16]
        return carry

    lax.fori_loop(0, SLABS, phase_b, 0)

    accp[...] = jnp.zeros((LANES, 96), F32)
    for a in range(KZ):
        accp[a * KY : (a + 1) * KY, :] = acc[a, 0:KY, :]
    o_ref[...] = dot(fx_ref[...], accp[...], NT)


def fold_kernel(p_ref, below_ref, above_ref, low_ref, high_ref, o_ref):
    total = p_ref[...]
    total += low_ref[...] * pltpu.roll(below_ref[...], LANES - 8, 1)
    total += high_ref[...] * pltpu.roll(above_ref[...], 8, 1)
    for member in range(MEMBERS):
        o_ref[member] = total


def power_kernel(g_ref, inv_ref, gx_ref, gzy_ref, o_ref):
    total = jnp.zeros((8, LANES), F32)
    for k in range(3):
        n = jnp.concatenate([g_ref[p, 8 * k : 8 * k + 8, :] for p in range(MEMBERS)], axis=0)
        n = n * inv_ref[...]
        t = dot(gx_ref[...], n, NN)
        u = dot(n, gzy_ref[...], NN)
        total += jnp.sum((t * u).reshape(MEMBERS, 8, LANES), axis=0)
    total = jnp.full((8, LANES), jnp.sum(total), F32)
    for stack in range(STACKS):
        o_ref[stack] = total


def field_kernel(size, g_ref, e_ref, w_ref, p_ref, o_ref):
    power = p_ref[0]
    for stack in range(1, STACKS):
        power = power + p_ref[stack]
    scale = 1.0 / (jnp.sqrt(power / size) + 1e-6)
    e = e_ref[...]
    for k in range(3):
        n = jnp.concatenate([g_ref[p, 8 * k : 8 * k + 8, :] for p in range(MEMBERS)], axis=0)
        h = dot(e, n, NT) * scale[0:1, 0:1]
        o_ref[k * LANES : (k + 1) * LANES, :] = dot(h, w_ref[...], NN)


def call(kernel, shapes, *args, scratch=()):
    return pl.pallas_call(
        kernel,
        out_shape=shapes,
        scratch_shapes=list(scratch),
        compiler_params=pltpu.CompilerParams(vmem_limit_bytes=48 << 20),
    )(*args)


def shards(fixed, moving):
    tab = tables()
    sds = lambda *shape: jax.ShapeDtypeStruct(shape, F32)
    stack = lax.axis_index("xy_0")
    slab = lax.axis_index(GZ)
    strip = lax.axis_index(("xy_1", "xy_2"))
    upward = [(i, i + 1) for i in range(STACKS - 1)]
    downward = [(i + 1, i) for i in range(STACKS - 1)]

    inverse = lax.dynamic_slice_in_dim(tab["inverse"], stack, 1, 0)
    ez = lax.dynamic_index_in_dim(tab["ez"], slab, 0, keepdims=False)
    ey = lax.dynamic_index_in_dim(tab["ey"], strip, 0, keepdims=False)
    evals = (ez[:, None, :] * ey[None, :, :]).reshape(LANES, LANES) * inverse

    flat = (DEPTH * ROWS, WIDTH)
    chunks = call(
        pack_kernel,
        sds(MEMBERS, 2, WIDE, LANES),
        fixed.reshape(flat),
        moving.reshape(flat),
        scratch=[
            pltpu.VMEM((2, WIDTH + 2 * RADIUS, LANES), F32),
            pltpu.VMEM((2, WIDTH // LANES, LANES, LANES), F32),
        ],
    )
    blocks = lax.all_to_all(chunks, PLANE, 0, 0)
    up, down = call(rim_kernel, (sds(2, 2, WIDE, LANES), sds(2, 2, WIDE, LANES)), blocks)
    below = lax.ppermute(up, "xy_0", upward)
    above = lax.ppermute(down, "xy_0", downward)
    part = call(
        force_kernel,
        sds(24, LANES),
        blocks,
        below,
        above,
        tab["fit_zy"],
        tab["fit_x"],
        scratch=[
            pltpu.VMEM((SLABS + 1, STRIPS + 1, 5, COLS, LANES), F32),
            pltpu.VMEM((SLABS + 1, STRIPS + 1, 5, COLS, LANES), F32),
            pltpu.VMEM((SLABS, 2, WIDE, LANES), F32),
            pltpu.VMEM((5, STRIPS, COLS, LANES), F32),
            pltpu.VMEM((96, STRIPS * LANES), F32),
            pltpu.VMEM((KZ, 16, 96), F32),
            pltpu.VMEM((LANES, 96), F32),
        ],
    )
    below = lax.ppermute(part, "xy_0", upward)
    above = lax.ppermute(part, "xy_0", downward)
    copies = call(
        fold_kernel,
        sds(MEMBERS, 24, LANES),
        part,
        below,
        above,
        tab["low"][None],
        tab["high"][None],
    )
    numer = lax.all_to_all(copies, PLANE, 0, 0)
    power = call(
        power_kernel, sds(STACKS, 8, LANES), numer, inverse, tab["gram_x"], tab["gram_zy"]
    )
    powers = lax.all_to_all(power, "xy_0", 0, 0)
    size = float(3 * SLABS * DEPTH * STACKS * STRIPS * ROWS * WIDTH)
    field = call(
        functools.partial(field_kernel, size),
        sds(3 * LANES, WIDTH),
        numer,
        evals,
        tab["wide_x"],
        powers,
    )
    return field.reshape(3, DEPTH, ROWS, WIDTH)


def solution(mesh):
    torus = Mesh(mesh.devices.reshape(4, 2, 16, 2, 2), ("gz_0", "gz_1", "xy_0", "xy_1", "xy_2"))
    placed = (P(GZ, XY, None), P(GZ, XY, None))
    return jax.shard_map(
        shards, mesh=torus, in_specs=placed, out_specs=P(None, GZ, XY, None), check_vma=False
    )
```

```python
import functools

import jax
import jax.numpy as jnp
import numpy as np
from jax import lax
from jax.experimental import pallas as pl
from jax.experimental.pallas import tpu as pltpu
from jax.sharding import Mesh
from jax.sharding import PartitionSpec as P

RADIUS = 4
SPACING = 8
EPS = 1e-05
COUNT = float((2 * RADIUS + 1) ** 3)
XY = ("xy_0", "xy_1", "xy_2")
GZ = ("gz_0", "gz_1")
PLANE = ("gz_0", "gz_1", "xy_1", "xy_2")
SLABS, STRIPS, STACKS = 8, 4, 16
MEMBERS = SLABS * STRIPS
DEPTH, ROWS, WIDTH = 8, 16, 1024
COLS = WIDTH // MEMBERS
WIDE = COLS + 2 * RADIUS
LANES = 128
KZ = SLABS + 3
KY = STRIPS * ROWS // SPACING + 3
F32 = jnp.float32
BF16 = jnp.bfloat16


def np_basis(index, knot):
    span = index // SPACING
    t = (index - span * SPACING) / SPACING
    j = knot - span
    out = np.where(j == 0, (1 - t) ** 3 / 6, 0.0)
    out = np.where(j == 1, (3 * t**3 - 6 * t**2 + 4) / 6, out)
    out = np.where(j == 2, (-3 * t**3 + 3 * t**2 + 3 * t + 1) / 6, out)
    return np.where(j == 3, t**3 / 6, out)


def np_fit(index, knot):
    value = np_basis(index, knot)
    span = index // SPACING
    total = sum(np_basis(index, span + step) ** 2 for step in range(4))
    return value**3 / total


def np_mass(knots, extent):
    spans = extent // SPACING
    within = np.arange(SPACING)
    energy = [np.sum(np_basis(within, np.full(SPACING, j)) ** 2) for j in range(4)]
    return np.array(
        [sum(energy[j] for j in range(4) if 0 <= c - j <= spans - 1) for c in range(knots)]
    )


def tables():
    z8, y16 = np.arange(DEPTH), np.arange(ROWS)
    fit_z = np_fit(z8[None, :], np.arange(4)[:, None])
    fit_y = np_fit(y16[None, :], np.arange(8)[:, None])
    fit_zy = np.einsum("az,by->abyz", fit_z, fit_y).reshape(32, LANES).astype(np.float32)
    fit_x = np_fit(np.arange(COLS)[None, :], np.arange(8)[:, None])
    fit_x = np.einsum("qr,kj,cx->qkcjrx", np.eye(STRIPS), np.eye(3), fit_x).reshape(96, 3 * LANES)
    place = np.zeros((STRIPS, 16, 8, LANES))
    for q in range(STRIPS):
        for a in range(KZ):
            for b in range(5):
                place[q, a, b, KY * a + 2 * q + b] = 1.0
    place = place.reshape(STRIPS, LANES, LANES)
    knots_x = WIDTH // SPACING + 3
    mass_x = np_mass(knots_x, WIDTH)
    full_x = np_basis(np.arange(WIDTH)[None, :], np.arange(knots_x)[:, None]) / mass_x[:, None]
    wide_x = np.zeros((MEMBERS, 8, WIDTH))
    for member in range(MEMBERS):
        wide_x[member, :7] = full_x[4 * member : 4 * member + 7]
    wide_x = wide_x.reshape(MEMBERS * 8, WIDTH)
    gram_x = wide_x @ wide_x.T
    eval_z = np_basis(np.arange(SLABS * DEPTH)[:, None], np.arange(KZ)[None, :])
    eval_y = np_basis(np.arange(STRIPS * ROWS)[:, None], np.arange(KY)[None, :])
    gram_zy = np.zeros((LANES, LANES))
    gram_zy[: KZ * KY, : KZ * KY] = np.kron(eval_z.T @ eval_z, eval_y.T @ eval_y)
    mass_z = np_mass(KZ, SLABS * DEPTH)
    mass_y = np_mass(STACKS * 8 + 3, STACKS * STRIPS * ROWS)
    inverse = np.zeros((STACKS, LANES))
    for stack in range(STACKS):
        inverse[stack, : KZ * KY] = (
            1.0 / (mass_z[:, None] * mass_y[None, 8 * stack : 8 * stack + KY])
        ).reshape(-1)
    ez = eval_z.reshape(SLABS, DEPTH, KZ)
    ey = eval_y.reshape(STRIPS, ROWS, KY)
    lane = np.arange(LANES)
    low = np.where((lane < KZ * KY) & (lane % KY < 3), 1.0, 0.0)
    high = np.where((lane < KZ * KY) & (lane % KY >= 8), 1.0, 0.0)
    ez_l = np.zeros((SLABS, DEPTH, LANES))
    ey_l = np.zeros((STRIPS, ROWS, LANES))
    ez_l[..., : KZ * KY] = np.repeat(ez, KY, axis=2)
    ey_l[..., : KZ * KY] = np.tile(ey, (1, 1, KZ))
    f = lambda v: np.asarray(v, np.float32)
    high_zy = fit_zy.astype(jnp.bfloat16)
    low_zy = (fit_zy - high_zy.astype(np.float32)).astype(jnp.bfloat16)
    fit_zy = np.block([[high_zy, high_zy], [low_zy, np.zeros_like(low_zy)]])
    return dict(
        fit_zy=fit_zy, place=f(place), fit_x=f(fit_x), wide_x=f(wide_x), gram_x=f(gram_x), gram_zy=f(gram_zy),
        inverse=f(inverse), ez=f(ez_l), ey=f(ey_l), low=f(low), high=f(high),
    )


def split(x):
    hi = x.astype(BF16)
    return hi, (x - hi.astype(F32)).astype(BF16)


def dot(a, b, dims):
    ah, al = split(a)
    bh, bl = split(b)
    d = lambda u, v: lax.dot_general(u, v, (dims, ((), ())), preferred_element_type=F32)
    return d(ah, bh) + d(ah, bl) + d(al, bh)


NN = ((1,), (0,))
NT = ((1,), (1,))


def pack_kernel(f_ref, m_ref, o_ref, s_ref, b_ref):
    zero = jnp.zeros((RADIUS, LANES), F32)
    for image, ref in enumerate((f_ref, m_ref)):
        s_ref[image, 0:RADIUS, :] = zero
        s_ref[image, RADIUS + WIDTH : 2 * RADIUS + WIDTH, :] = zero
        for block in range(WIDTH // LANES):
            buf = b_ref.at[image, block]
            buf[...] = ref[:, block * LANES : (block + 1) * LANES]
            rows = [buf[pl.ds(y, DEPTH, stride=ROWS), :] for y in range(ROWS)]
            tile = jnp.concatenate(rows, axis=0).T
            s_ref[image, RADIUS + block * LANES : RADIUS + (block + 1) * LANES, :] = tile
    for image in range(2):
        for member in range(MEMBERS):
            o_ref[member, image] = s_ref[image, member * COLS : member * COLS + WIDE, :]


def rim_kernel(r_ref, up_ref, down_ref):
    for half in range(2):
        for image in range(2):
            slabs = range(4 * half, 4 * half + 4)
            up_ref[half, image] = jnp.concatenate(
                [r_ref[STRIPS * g + STRIPS - 1, image, :, 96:128] for g in slabs], axis=1
            )
            down_ref[half, image] = jnp.concatenate(
                [r_ref[STRIPS * g, image, :, 0:32] for g in slabs], axis=1
            )


def force_kernel(
    r_ref, below_ref, above_ref, fz_ref, fx_ref, place_ref, o_ref, stack, rim_t, turned, mid, fr, acc
):
    roll = pltpu.roll

    def window_x(v):
        s = v + roll(v, WIDE - 1, 0)
        s = s + roll(s, WIDE - 2, 0)
        s = s + roll(s, WIDE - 4, 0)
        return s[0:COLS] + v[2 * RADIUS : 2 * RADIUS + COLS]

    def windows(f, m):
        return [window_x(v) for v in (f, m, f * f, m * m, f * m)]

    for half in range(2):
        for at, ref in ((0, below_ref), (96, above_ref)):
            values = windows(ref[half, 0], ref[half, 1])
            values.append(ref[half, 1, RADIUS : RADIUS + COLS, :])
            for item, v in enumerate(values):
                stack[item, at : at + COLS, :] = v
        for item in range(6):
            stack[item, 32:96, :] = jnp.zeros((64, LANES), F32)
            rim_t[half, item] = stack[item].T

    def phase_x(g, carry):
        for q in range(STRIPS):
            i = g * STRIPS + q
            values = windows(r_ref[i, 0], r_ref[i, 1])
            values.append(r_ref[i, 0, RADIUS : RADIUS + COLS, :])
            values.append(r_ref[i, 1, RADIUS : RADIUS + COLS, :])
            values.append(
                (
                    r_ref[i, 1, RADIUS + 1 : RADIUS + 1 + COLS, :]
                    - r_ref[i, 1, RADIUS - 1 : RADIUS - 1 + COLS, :]
                )
                * 0.5
            )
            for item, v in enumerate(values):
                stack[item, q * COLS : (q + 1) * COLS, :] = v
        for item in range(8):
            turned[item, g] = stack[item].T
        return carry

    lax.fori_loop(0, SLABS, phase_x, 0)

    lane = lax.broadcasted_iota(jnp.int32, (8, LANES), 1)
    first, last = lane < COLS, lane >= LANES - COLS
    row = lambda y: pl.ds(y * 8, 8) if not isinstance(y, int) else slice(y * 8, y * 8 + 8)

    def phase_y(g, carry):
        half = g // 4
        base = (g % 4) * 4
        near = lambda item, i: rim_t[half, item, row(base + i), :]
        for field in range(5):
            v = [turned[field, g, row(y), :] for y in range(ROWS)]
            lower = [jnp.where(first, near(field, i), roll(v[12 + i], COLS, 1)) for i in range(4)]
            upper = [jnp.where(last, near(field, i), roll(v[i], LANES - COLS, 1)) for i in range(4)]
            v = lower + v + upper
            s = [v[i] + v[i + 1] for i in range(23)]
            s = [s[i] + s[i + 2] for i in range(21)]
            for y in range(ROWS):
                turned[field, g, row(y), :] = (s[y] + s[y + 4]) + v[y + 8]
        m0 = turned[6, g, row(0), :]
        m15 = turned[6, g, row(15), :]
        mid[g, row(0), :] = jnp.where(first, near(5, 3), roll(m15, COLS, 1))
        mid[g, row(17), :] = jnp.where(last, near(5, 0), roll(m0, LANES - COLS, 1))
        mid[g, 8 : 8 + LANES, :] = turned[6, g]
        return carry

    lax.fori_loop(0, SLABS, phase_y, 0)

    z = lax.broadcasted_iota(jnp.int32, (8, LANES), 0)
    zero = jnp.zeros((8, LANES), F32)

    def window_z(v):
        v = [zero] + v + [zero]

        def ahead(u, d):
            r = [roll(x, 8 - d, 0) for x in u] + [zero]
            return [x + jnp.where(z < 8 - d, r[i], r[i + 1]) for i, x in enumerate(u)]

        s = ahead(ahead(ahead(v, 1), 2), 4)
        t = [s[i] + v[i + 1] for i in range(SLABS + 1)]
        return [roll(jnp.where(z >= 4, t[g], t[g + 1]), 4, 0) for g in range(SLABS)]

    inv = 1.0 / COUNT

    def phase_z(y, carry):
        sums = [window_z([turned[field, g, row(y), :] for g in range(SLABS)]) for field in range(5)]
        m = [mid[g, row(y + 1), :] for g in range(SLABS)]
        fore = [roll(v, 7, 0) for v in m] + [zero]
        back = [zero] + [roll(v, 1, 0) for v in m]
        for g in range(SLABS):
            grad_z = (
                jnp.where(z < 7, fore[g], fore[g + 1]) - jnp.where(z > 0, back[g + 1], back[g])
            ) * 0.5
            grad_y = (mid[g, row(y + 2), :] - mid[g, row(y), :]) * 0.5
            grad_x = turned[7, g, row(y), :]
            mean_f = sums[0][g] * inv
            mean_m = sums[1][g] * inv
            cov = sums[4][g] * inv - mean_f * mean_m
            var_f = sums[2][g] * inv - mean_f * mean_f
            var_m = sums[3][g] * inv - mean_m * mean_m
            factor = 2.0 * cov / (var_f * var_m + EPS)
            resid = turned[5, g, row(y), :] - mean_f - cov / (var_m + EPS) * (m[g] - mean_m)
            common = factor * resid
            for k, grad in enumerate((grad_z, grad_y, grad_x)):
                fr[g, row(y), k * LANES : (k + 1) * LANES] = common * grad
        return carry

    lax.fori_loop(0, ROWS, phase_z, 0)

    acc[...] = jnp.zeros((16, 8, 3 * LANES), F32)
    for g in range(SLABS):
        hi, lo = split(fr[g])
        part = lax.dot_general(
            fz_ref[...], jnp.concatenate([hi, lo], axis=0), (NN, ((), ())), preferred_element_type=F32
        )
        for a in range(4):
            acc[g + a] += part[8 * a : 8 * a + 8] + part[32 + 8 * a : 40 + 8 * a]
    wide = dot(fx_ref[...], acc[...].reshape(LANES, 3 * LANES), NT)
    total = dot(wide[0:24], place_ref[0], NN)
    for q in range(1, STRIPS):
        total += dot(wide[24 * q : 24 * q + 24], place_ref[q], NN)
    o_ref[...] = total


def fold_kernel(p_ref, below_ref, above_ref, low_ref, high_ref, o_ref):
    total = p_ref[...]
    total += low_ref[...] * pltpu.roll(below_ref[...], LANES - 8, 1)
    total += high_ref[...] * pltpu.roll(above_ref[...], 8, 1)
    for member in range(MEMBERS):
        o_ref[member] = total


def power_kernel(g_ref, inv_ref, gx_ref, gzy_ref, o_ref):
    total = jnp.zeros((8, LANES), F32)
    for k in range(3):
        n = jnp.concatenate([g_ref[p, 8 * k : 8 * k + 8, :] for p in range(MEMBERS)], axis=0)
        n = n * inv_ref[...]
        t = dot(gx_ref[...], n, NN)
        u = dot(n, gzy_ref[...], NN)
        total += jnp.sum((t * u).reshape(MEMBERS, 8, LANES), axis=0)
    total = jnp.full((8, LANES), jnp.sum(total), F32)
    for stack in range(STACKS):
        o_ref[stack] = total


def field_kernel(size, g_ref, e_ref, w_ref, p_ref, o_ref):
    power = p_ref[0]
    for stack in range(1, STACKS):
        power = power + p_ref[stack]
    scale = 1.0 / (jnp.sqrt(power / size) + 1e-6)
    e = e_ref[...]
    for k in range(3):
        n = jnp.concatenate([g_ref[p, 8 * k : 8 * k + 8, :] for p in range(MEMBERS)], axis=0)
        h = dot(e, n, NT) * scale[0:1, 0:1]
        o_ref[k * LANES : (k + 1) * LANES, :] = dot(h, w_ref[...], NN)


def call(kernel, shapes, *args, scratch=()):
    return pl.pallas_call(
        kernel,
        out_shape=shapes,
        scratch_shapes=list(scratch),
        compiler_params=pltpu.CompilerParams(vmem_limit_bytes=48 << 20),
    )(*args)


def shards(fixed, moving):
    tab = tables()
    sds = lambda *shape: jax.ShapeDtypeStruct(shape, F32)
    stack = lax.axis_index("xy_0")
    slab = lax.axis_index(GZ)
    strip = lax.axis_index(("xy_1", "xy_2"))
    upward = [(i, i + 1) for i in range(STACKS - 1)]
    downward = [(i + 1, i) for i in range(STACKS - 1)]

    inverse = lax.dynamic_slice_in_dim(tab["inverse"], stack, 1, 0)
    ez = lax.dynamic_index_in_dim(tab["ez"], slab, 0, keepdims=False)
    ey = lax.dynamic_index_in_dim(tab["ey"], strip, 0, keepdims=False)
    evals = (ez[:, None, :] * ey[None, :, :]).reshape(LANES, LANES) * inverse

    flat = (DEPTH * ROWS, WIDTH)
    chunks = call(
        pack_kernel,
        sds(MEMBERS, 2, WIDE, LANES),
        fixed.reshape(flat),
        moving.reshape(flat),
        scratch=[
            pltpu.VMEM((2, WIDTH + 2 * RADIUS, LANES), F32),
            pltpu.VMEM((2, WIDTH // LANES, LANES, LANES), F32),
        ],
    )
    blocks = lax.all_to_all(chunks, PLANE, 0, 0)
    up, down = call(rim_kernel, (sds(2, 2, WIDE, LANES), sds(2, 2, WIDE, LANES)), blocks)
    below = lax.ppermute(up, "xy_0", upward)
    above = lax.ppermute(down, "xy_0", downward)
    part = call(
        force_kernel,
        sds(24, LANES),
        blocks,
        below,
        above,
        tab["fit_zy"],
        tab["fit_x"],
        tab["place"],
        scratch=[
            pltpu.VMEM((8, LANES, LANES), F32),
            pltpu.VMEM((2, 6, LANES, LANES), F32),
            pltpu.VMEM((8, SLABS, LANES, LANES), F32),
            pltpu.VMEM((SLABS, LANES + 16, LANES), F32),
            pltpu.VMEM((SLABS, LANES, 3 * LANES), F32),
            pltpu.VMEM((16, 8, 3 * LANES), F32),
        ],
    )
    below = lax.ppermute(part, "xy_0", upward)
    above = lax.ppermute(part, "xy_0", downward)
    copies = call(
        fold_kernel,
        sds(MEMBERS, 24, LANES),
        part,
        below,
        above,
        tab["low"][None],
        tab["high"][None],
    )
    numer = lax.all_to_all(copies, PLANE, 0, 0)
    power = call(
        power_kernel, sds(STACKS, 8, LANES), numer, inverse, tab["gram_x"], tab["gram_zy"]
    )
    powers = lax.all_to_all(power, "xy_0", 0, 0)
    size = float(3 * SLABS * DEPTH * STACKS * STRIPS * ROWS * WIDTH)
    field = call(
        functools.partial(field_kernel, size),
        sds(3 * LANES, WIDTH),
        numer,
        evals,
        tab["wide_x"],
        powers,
    )
    return field.reshape(3, DEPTH, ROWS, WIDTH)


def solution(mesh):
    torus = Mesh(mesh.devices.reshape(4, 2, 16, 2, 2), ("gz_0", "gz_1", "xy_0", "xy_1", "xy_2"))
    placed = (P(GZ, XY, None), P(GZ, XY, None))
    return jax.shard_map(
        shards, mesh=torus, in_specs=placed, out_specs=P(None, GZ, XY, None), check_vma=False
    )
```

```python
import functools

import jax
import jax.numpy as jnp
import numpy as np
from jax import lax
from jax.experimental import pallas as pl
from jax.experimental.pallas import tpu as pltpu
from jax.sharding import Mesh
from jax.sharding import PartitionSpec as P

RADIUS = 4
SPACING = 8
EPS = 1e-05
COUNT = float((2 * RADIUS + 1) ** 3)
XY = ("xy_0", "xy_1", "xy_2")
GZ = ("gz_0", "gz_1")
PLANE = ("gz_0", "gz_1", "xy_1", "xy_2")


def member_of(slab, strip):
    place = {"gz_0": slab // 2, "gz_1": slab % 2, "xy_1": strip // 2, "xy_2": strip % 2}
    size = {"gz_0": 4, "gz_1": 2, "xy_1": 2, "xy_2": 2}
    return functools.reduce(lambda total, axis: total * size[axis] + place[axis], PLANE, 0)


SLABS, STRIPS, STACKS = 8, 4, 16
MEMBERS = SLABS * STRIPS
DEPTH, ROWS, WIDTH = 8, 16, 1024
COLS = WIDTH // MEMBERS
FROM_MIDDLE = sorted(range(STACKS), key=lambda i: abs(2 * i - STACKS))
WIDE = COLS + 2 * RADIUS
LANES = 128
KZ = SLABS + 3
KY = STRIPS * ROWS // SPACING + 3
F32 = jnp.float32
BF16 = jnp.bfloat16


def np_basis(index, knot):
    span = index // SPACING
    t = (index - span * SPACING) / SPACING
    j = knot - span
    out = np.where(j == 0, (1 - t) ** 3 / 6, 0.0)
    out = np.where(j == 1, (3 * t**3 - 6 * t**2 + 4) / 6, out)
    out = np.where(j == 2, (-3 * t**3 + 3 * t**2 + 3 * t + 1) / 6, out)
    return np.where(j == 3, t**3 / 6, out)


def np_fit(index, knot):
    value = np_basis(index, knot)
    span = index // SPACING
    total = sum(np_basis(index, span + step) ** 2 for step in range(4))
    return value**3 / total


def np_mass(knots, extent):
    spans = extent // SPACING
    within = np.arange(SPACING)
    energy = [np.sum(np_basis(within, np.full(SPACING, j)) ** 2) for j in range(4)]
    return np.array(
        [sum(energy[j] for j in range(4) if 0 <= c - j <= spans - 1) for c in range(knots)]
    )


def tables():
    z8, y16 = np.arange(DEPTH), np.arange(ROWS)
    fit_z = np_fit(z8[None, :], np.arange(4)[:, None])
    fit_y = np_fit(y16[None, :], np.arange(8)[:, None])
    fit_zy = np.einsum("az,by->abyz", fit_z, fit_y).reshape(32, LANES).astype(np.float32)
    fit_x = np_fit(np.arange(COLS)[None, :], np.arange(8)[:, None])
    fit_x = np.einsum("qr,kj,cx->qkcjrx", np.eye(STRIPS), np.eye(3), fit_x).reshape(96, 3 * LANES)
    place = np.zeros((STRIPS, 16, 8, LANES))
    for q in range(STRIPS):
        for a in range(KZ):
            for b in range(5):
                place[q, a, b, KY * a + 2 * q + b] = 1.0
    place = place.reshape(STRIPS, LANES, LANES)
    knots_x = WIDTH // SPACING + 3
    mass_x = np_mass(knots_x, WIDTH)
    full_x = np_basis(np.arange(WIDTH)[None, :], np.arange(knots_x)[:, None]) / mass_x[:, None]
    wide_x = np.zeros((MEMBERS, 8, WIDTH))
    for member in range(MEMBERS):
        wide_x[member, :7] = full_x[4 * member : 4 * member + 7]
    wide_x = wide_x.reshape(MEMBERS * 8, WIDTH)
    gram_x = wide_x @ wide_x.T
    eval_z = np_basis(np.arange(SLABS * DEPTH)[:, None], np.arange(KZ)[None, :])
    eval_y = np_basis(np.arange(STRIPS * ROWS)[:, None], np.arange(KY)[None, :])
    gram_zy = np.zeros((LANES, LANES))
    gram_zy[: KZ * KY, : KZ * KY] = np.kron(eval_z.T @ eval_z, eval_y.T @ eval_y)
    mass_z = np_mass(KZ, SLABS * DEPTH)
    mass_y = np_mass(STACKS * 8 + 3, STACKS * STRIPS * ROWS)
    inverse = np.zeros((STACKS, LANES))
    for stack in range(STACKS):
        inverse[stack, : KZ * KY] = (
            1.0 / (mass_z[:, None] * mass_y[None, 8 * stack : 8 * stack + KY])
        ).reshape(-1)
    ez = eval_z.reshape(SLABS, DEPTH, KZ)
    ey = eval_y.reshape(STRIPS, ROWS, KY)
    lane = np.arange(LANES)
    low = np.where((lane < KZ * KY) & (lane % KY < 3), 1.0, 0.0)
    high = np.where((lane < KZ * KY) & (lane % KY >= 8), 1.0, 0.0)
    ez_l = np.zeros((SLABS, DEPTH, LANES))
    ey_l = np.zeros((STRIPS, ROWS, LANES))
    ez_l[..., : KZ * KY] = np.repeat(ez, KY, axis=2)
    ey_l[..., : KZ * KY] = np.tile(ey, (1, 1, KZ))
    f = lambda v: np.asarray(v, np.float32)
    high_zy = fit_zy.astype(jnp.bfloat16)
    low_zy = (fit_zy - high_zy.astype(np.float32)).astype(jnp.bfloat16)
    fit_zy = np.block([[high_zy, high_zy], [low_zy, np.zeros_like(low_zy)]])
    return dict(
        fit_zy=fit_zy, place=f(place), fit_x=f(fit_x), wide_x=f(wide_x), gram_x=f(gram_x), gram_zy=f(gram_zy),
        inverse=f(inverse), ez=f(ez_l), ey=f(ey_l), low=f(low), high=f(high),
    )


def split(x):
    hi = x.astype(BF16)
    return hi, (x - hi.astype(F32)).astype(BF16)


def dot(a, b, dims):
    ah, al = split(a)
    bh, bl = split(b)
    d = lambda u, v: lax.dot_general(u, v, (dims, ((), ())), preferred_element_type=F32)
    return d(ah, bh) + d(ah, bl) + d(al, bh)


NN = ((1,), (0,))
NT = ((1,), (1,))


def pack_kernel(f_ref, m_ref, o_ref, s_ref, b_ref, t_ref, sem):
    copies = [
        pltpu.make_async_copy(ref, b_ref.at[image], sem.at[image])
        for image, ref in enumerate((f_ref, m_ref))
    ]
    for copy in copies:
        copy.start()
    zero = jnp.zeros((RADIUS, LANES), F32)
    for image in range(2):
        s_ref[image, 0:RADIUS, :] = zero
        s_ref[image, RADIUS + WIDTH : 2 * RADIUS + WIDTH, :] = zero
    for image in range(2):
        copies[image].wait()
        for block in range(WIDTH // LANES):
            buf = t_ref.at[image, block]
            buf[...] = b_ref[image, :, block * LANES : (block + 1) * LANES]
            rows = [buf[pl.ds(y, DEPTH, stride=ROWS), :] for y in range(ROWS)]
            tile = jnp.concatenate(rows, axis=0).T
            s_ref[image, RADIUS + block * LANES : RADIUS + (block + 1) * LANES, :] = tile
        for member in range(MEMBERS):
            o_ref[member, image] = s_ref[image, member * COLS : member * COLS + WIDE, :]


def rim_kernel(r_ref, up_ref, down_ref):
    for half in range(2):
        for image in range(2):
            slabs = range(4 * half, 4 * half + 4)
            up_ref[half, image] = jnp.concatenate(
                [r_ref[member_of(g, STRIPS - 1), image, :, 96:128] for g in slabs], axis=1
            )
            down_ref[half, image] = jnp.concatenate(
                [r_ref[member_of(g, 0), image, :, 0:32] for g in slabs], axis=1
            )


def window_x(v):
    roll = pltpu.roll
    s = v + roll(v, WIDE - 1, 0)
    s = s + roll(s, WIDE - 2, 0)
    s = s + roll(s, WIDE - 4, 0)
    return s[0:COLS] + v[2 * RADIUS : 2 * RADIUS + COLS]


def windows(f, m):
    return [window_x(v) for v in (f, m, f * f, m * m, f * m)]


def columns_kernel(r_ref, turned, stack):
    def phase_x(g, carry):
        for q in range(STRIPS):
            i = member_of(g, q)
            values = windows(r_ref[i, 0], r_ref[i, 1])
            values.append(r_ref[i, 0, RADIUS : RADIUS + COLS, :])
            values.append(r_ref[i, 1, RADIUS : RADIUS + COLS, :])
            values.append(
                (
                    r_ref[i, 1, RADIUS + 1 : RADIUS + 1 + COLS, :]
                    - r_ref[i, 1, RADIUS - 1 : RADIUS - 1 + COLS, :]
                )
                * 0.5
            )
            for item, v in enumerate(values):
                stack[item, q * COLS : (q + 1) * COLS, :] = v
        for item in range(8):
            turned[item, g] = stack[item].T
        return carry

    lax.fori_loop(0, SLABS, phase_x, 0)


def force_kernel(
    turned, below_ref, above_ref, fz_ref, fx_ref, place_ref, o_ref, stack, rim_t, summed, mid, fr, acc
):
    roll = pltpu.roll

    for half in range(2):
        for at, ref in ((0, below_ref), (96, above_ref)):
            values = windows(ref[half, 0], ref[half, 1])
            values.append(ref[half, 1, RADIUS : RADIUS + COLS, :])
            for item, v in enumerate(values):
                stack[item, at : at + COLS, :] = v
        for item in range(6):
            stack[item, 32:96, :] = jnp.zeros((64, LANES), F32)
            rim_t[half, item] = stack[item].T

    lane = lax.broadcasted_iota(jnp.int32, (8, LANES), 1)
    first, last = lane < COLS, lane >= LANES - COLS
    row = lambda y: pl.ds(y * 8, 8) if not isinstance(y, int) else slice(y * 8, y * 8 + 8)

    def phase_y(g, carry):
        half = g // 4
        base = (g % 4) * 4
        near = lambda item, i: rim_t[half, item, row(base + i), :]
        for field in range(5):
            v = [turned[field, g, row(y), :] for y in range(ROWS)]
            lower = [jnp.where(first, near(field, i), roll(v[12 + i], COLS, 1)) for i in range(4)]
            upper = [jnp.where(last, near(field, i), roll(v[i], LANES - COLS, 1)) for i in range(4)]
            v = lower + v + upper
            s = [v[i] + v[i + 1] for i in range(23)]
            s = [s[i] + s[i + 2] for i in range(21)]
            for y in range(ROWS):
                summed[field, g, row(y), :] = (s[y] + s[y + 4]) + v[y + 8]
        m0 = turned[6, g, row(0), :]
        m15 = turned[6, g, row(15), :]
        mid[g, row(0), :] = jnp.where(first, near(5, 3), roll(m15, COLS, 1))
        mid[g, row(17), :] = jnp.where(last, near(5, 0), roll(m0, LANES - COLS, 1))
        mid[g, 8 : 8 + LANES, :] = turned[6, g]
        return carry

    lax.fori_loop(0, SLABS, phase_y, 0)

    z = lax.broadcasted_iota(jnp.int32, (8, LANES), 0)
    zero = jnp.zeros((8, LANES), F32)

    def window_z(v):
        v = [zero] + v + [zero]

        def ahead(u, d):
            r = [roll(x, 8 - d, 0) for x in u] + [zero]
            return [x + jnp.where(z < 8 - d, r[i], r[i + 1]) for i, x in enumerate(u)]

        s = ahead(ahead(ahead(v, 1), 2), 4)
        t = [s[i] + v[i + 1] for i in range(SLABS + 1)]
        return [roll(jnp.where(z >= 4, t[g], t[g + 1]), 4, 0) for g in range(SLABS)]

    inv = 1.0 / COUNT

    def phase_z(y, carry):
        sums = [window_z([summed[field, g, row(y), :] for g in range(SLABS)]) for field in range(5)]
        m = [mid[g, row(y + 1), :] for g in range(SLABS)]
        fore = [roll(v, 7, 0) for v in m] + [zero]
        back = [zero] + [roll(v, 1, 0) for v in m]
        for g in range(SLABS):
            grad_z = (
                jnp.where(z < 7, fore[g], fore[g + 1]) - jnp.where(z > 0, back[g + 1], back[g])
            ) * 0.5
            grad_y = (mid[g, row(y + 2), :] - mid[g, row(y), :]) * 0.5
            grad_x = turned[7, g, row(y), :]
            mean_f = sums[0][g] * inv
            mean_m = sums[1][g] * inv
            cov = sums[4][g] * inv - mean_f * mean_m
            var_f = sums[2][g] * inv - mean_f * mean_f
            var_m = sums[3][g] * inv - mean_m * mean_m
            factor = 2.0 * cov / (var_f * var_m + EPS)
            resid = turned[5, g, row(y), :] - mean_f - cov / (var_m + EPS) * (m[g] - mean_m)
            common = factor * resid
            for k, grad in enumerate((grad_z, grad_y, grad_x)):
                fr[g, row(y), k * LANES : (k + 1) * LANES] = common * grad
        return carry

    lax.fori_loop(0, ROWS, phase_z, 0)

    acc[...] = jnp.zeros((16, 8, 3 * LANES), F32)
    for g in range(SLABS):
        hi, lo = split(fr[g])
        part = lax.dot_general(
            fz_ref[...], jnp.concatenate([hi, lo], axis=0), (NN, ((), ())), preferred_element_type=F32
        )
        for a in range(4):
            acc[g + a] += part[8 * a : 8 * a + 8] + part[32 + 8 * a : 40 + 8 * a]
    wide = dot(fx_ref[...], acc[...].reshape(LANES, 3 * LANES), NT)
    total = dot(wide[0:24], place_ref[0], NN)
    for q in range(1, STRIPS):
        total += dot(wide[24 * q : 24 * q + 24], place_ref[q], NN)
    o_ref[...] = total


def fold_kernel(p_ref, below_ref, above_ref, low_ref, high_ref, o_ref):
    total = p_ref[...]
    total += low_ref[...] * pltpu.roll(below_ref[...], LANES - 8, 1)
    total += high_ref[...] * pltpu.roll(above_ref[...], 8, 1)
    for member in range(MEMBERS):
        o_ref[member] = total


def gathered(g_ref, k):
    return jnp.concatenate([g_ref[p, 8 * k : 8 * k + 8, :] for p in range(MEMBERS)], axis=0)


def power_kernel(g_ref, inv_ref, gx_ref, gzy_ref, o_ref):
    parts = [gathered(g_ref, k) * inv_ref[...] for k in range(3)]
    t = dot(gx_ref[...], jnp.concatenate(parts, axis=1), NN)
    u = dot(jnp.concatenate(parts, axis=0), gzy_ref[...], NN)
    total = jnp.zeros((8, LANES), F32)
    size = 8 * MEMBERS
    for k in range(3):
        product = t[:, k * LANES : (k + 1) * LANES] * u[k * size : (k + 1) * size]
        total += jnp.sum(product.reshape(MEMBERS, 8, LANES), axis=0)
    total = jnp.full((8, LANES), jnp.sum(total), F32)
    for stack in range(STACKS):
        o_ref[stack] = total


def field_kernel(g_ref, ez_ref, ey_ref, inv_ref, w_ref, o_ref):
    ey = ey_ref[...]
    rows = [ez_ref[z : z + 1] * ey for z in range(DEPTH)]
    e = jnp.concatenate(rows, axis=0) * inv_ref[...]
    h = dot(e, jnp.concatenate([gathered(g_ref, k) for k in range(3)], axis=0), NT)
    size = 8 * MEMBERS
    h = jnp.concatenate([h[:, k * size : (k + 1) * size] for k in range(3)], axis=0)
    o_ref[...] = dot(h, w_ref[...], NN)


def scale_kernel(size, f_ref, p_ref, o_ref):
    power = p_ref[0]
    for stack in range(1, STACKS):
        power = power + p_ref[stack]
    scale = 1.0 / (jnp.sqrt(power / size) + 1e-6)
    o_ref[...] = f_ref[...] * scale[0:1, 0:1]


def call(kernel, shapes, *args, scratch=(), flops=0, **kw):
    if flops:
        kw["cost_estimate"] = pl.CostEstimate(flops=flops, transcendentals=0, bytes_accessed=1 << 20)
    return pl.pallas_call(
        kernel,
        out_shape=shapes,
        scratch_shapes=list(scratch),
        compiler_params=pltpu.CompilerParams(vmem_limit_bytes=40 << 20),
        **kw,
    )(*args)


def shards(fixed, moving):
    tab = tables()
    sds = lambda *shape: jax.ShapeDtypeStruct(shape, F32)
    stack = lax.axis_index("xy_0")
    slab = lax.axis_index(GZ)
    strip = lax.axis_index(("xy_1", "xy_2"))
    upward = [(i, i + 1) for i in range(STACKS - 1)]
    downward = [(i + 1, i) for i in range(STACKS - 1)]

    inverse = lax.dynamic_slice_in_dim(tab["inverse"], stack, 1, 0)
    ez = lax.dynamic_index_in_dim(tab["ez"], slab, 0, keepdims=False)
    ey = lax.dynamic_index_in_dim(tab["ey"], strip, 0, keepdims=False)

    flat = (DEPTH * ROWS, WIDTH)
    chunks = call(
        pack_kernel,
        sds(MEMBERS, 2, WIDE, LANES),
        pltpu.with_memory_space_constraint(fixed.reshape(flat), pltpu.HBM),
        pltpu.with_memory_space_constraint(moving.reshape(flat), pltpu.HBM),
        scratch=[
            pltpu.VMEM((2, WIDTH + 2 * RADIUS, LANES), F32),
            pltpu.VMEM((2, LANES, WIDTH), F32),
            pltpu.VMEM((2, WIDTH // LANES, LANES, LANES), F32),
            pltpu.SemaphoreType.DMA((2,)),
        ],
        in_specs=[pl.BlockSpec(memory_space=pltpu.HBM)] * 2,
    )
    blocks = lax.all_to_all(chunks, PLANE, 0, 0)
    up, down = call(rim_kernel, (sds(2, 2, WIDE, LANES), sds(2, 2, WIDE, LANES)), blocks)
    below = lax.ppermute(up, "xy_0", upward)
    above = lax.ppermute(down, "xy_0", downward)
    turned = call(
        columns_kernel,
        sds(8, SLABS, LANES, LANES),
        blocks,
        scratch=[pltpu.VMEM((8, LANES, LANES), F32)],
        flops=1 << 31,
    )
    part = call(
        force_kernel,
        sds(24, LANES),
        turned,
        below,
        above,
        tab["fit_zy"],
        tab["fit_x"],
        tab["place"],
        scratch=[
            pltpu.VMEM((6, LANES, LANES), F32),
            pltpu.VMEM((2, 6, LANES, LANES), F32),
            pltpu.VMEM((5, SLABS, LANES, LANES), F32),
            pltpu.VMEM((SLABS, LANES + 16, LANES), F32),
            pltpu.VMEM((SLABS, LANES, 3 * LANES), F32),
            pltpu.VMEM((16, 8, 3 * LANES), F32),
        ],
    )
    below = lax.ppermute(part, "xy_0", upward)
    above = lax.ppermute(part, "xy_0", downward)
    copies = call(
        fold_kernel,
        sds(MEMBERS, 24, LANES),
        part,
        below,
        above,
        tab["low"][None],
        tab["high"][None],
    )
    numer = lax.all_to_all(copies, PLANE, 0, 0)
    power = call(
        power_kernel, sds(STACKS, 8, LANES), numer, inverse, tab["gram_x"], tab["gram_zy"]
    )
    powers = lax.all_to_all(power, "xy_0", 0, 0, axis_index_groups=[FROM_MIDDLE])
    size = float(3 * SLABS * DEPTH * STACKS * STRIPS * ROWS * WIDTH)
    field = call(
        field_kernel,
        sds(3 * LANES, WIDTH),
        numer,
        ez,
        ey,
        inverse,
        tab["wide_x"],
        flops=1 << 31,
    )
    block = (LANES, WIDTH)
    field = call(
        functools.partial(scale_kernel, size),
        sds(3 * LANES, WIDTH),
        field,
        powers,
        grid=(3,),
        in_specs=[
            pl.BlockSpec(block, lambda i: (i, 0)),
            pl.BlockSpec((STACKS, 8, LANES), lambda i: (0, 0, 0)),
        ],
        out_specs=pl.BlockSpec(block, lambda i: (i, 0)),
    )
    return field.reshape(3, DEPTH, ROWS, WIDTH)


def solution(mesh):
    torus = Mesh(mesh.devices.reshape(4, 2, 16, 2, 2), ("gz_0", "gz_1", "xy_0", "xy_1", "xy_2"))
    placed = (P(GZ, XY, None), P(GZ, XY, None))
    return jax.shard_map(
        shards, mesh=torus, in_specs=placed, out_specs=P(None, GZ, XY, None), check_vma=False
    )
```

```python
import functools

import jax
import jax.numpy as jnp
import numpy as np
from jax import lax
from jax.experimental import pallas as pl
from jax.experimental.pallas import tpu as pltpu
from jax.sharding import Mesh
from jax.sharding import PartitionSpec as P

RADIUS = 4
SPACING = 8
EPS = 1e-05
COUNT = float((2 * RADIUS + 1) ** 3)
XY = ("xy_0", "xy_1", "xy_2")
GZ = ("gz_0", "gz_1")
PLANE = ("gz_0", "gz_1", "xy_1", "xy_2")


def member_of(slab, strip):
    place = {"gz_0": slab // 2, "gz_1": slab % 2, "xy_1": strip // 2, "xy_2": strip % 2}
    size = {"gz_0": 4, "gz_1": 2, "xy_1": 2, "xy_2": 2}
    return functools.reduce(lambda total, axis: total * size[axis] + place[axis], PLANE, 0)


SLABS, STRIPS, STACKS = 8, 4, 16
MEMBERS = SLABS * STRIPS
DEPTH, ROWS, WIDTH = 8, 16, 1024
COLS = WIDTH // MEMBERS
FROM_MIDDLE = sorted(range(STACKS), key=lambda i: abs(2 * i - STACKS))
WIDE = COLS + 2 * RADIUS
LANES = 128
PARTS = 6
KZ = SLABS + 3
KY = STRIPS * ROWS // SPACING + 3
F32 = jnp.float32
BF16 = jnp.bfloat16


def np_basis(index, knot):
    span = index // SPACING
    t = (index - span * SPACING) / SPACING
    j = knot - span
    out = np.where(j == 0, (1 - t) ** 3 / 6, 0.0)
    out = np.where(j == 1, (3 * t**3 - 6 * t**2 + 4) / 6, out)
    out = np.where(j == 2, (-3 * t**3 + 3 * t**2 + 3 * t + 1) / 6, out)
    return np.where(j == 3, t**3 / 6, out)


def np_fit(index, knot):
    value = np_basis(index, knot)
    span = index // SPACING
    total = sum(np_basis(index, span + step) ** 2 for step in range(4))
    return value**3 / total


def np_mass(knots, extent):
    spans = extent // SPACING
    within = np.arange(SPACING)
    energy = [np.sum(np_basis(within, np.full(SPACING, j)) ** 2) for j in range(4)]
    return np.array(
        [sum(energy[j] for j in range(4) if 0 <= c - j <= spans - 1) for c in range(knots)]
    )


def tables():
    z8, y16 = np.arange(DEPTH), np.arange(ROWS)
    fit_z = np_fit(z8[None, :], np.arange(4)[:, None])
    fit_y = np_fit(y16[None, :], np.arange(8)[:, None])
    fit_zy = np.einsum("az,by->abyz", fit_z, fit_y).reshape(32, LANES).astype(np.float32)
    fit_x = np_fit(np.arange(COLS)[None, :], np.arange(8)[:, None])
    fit_x = np.einsum("qr,kj,cx->qkcjrx", np.eye(STRIPS), np.eye(3), fit_x).reshape(96, 3 * LANES)
    place = np.zeros((STRIPS, 16, 8, LANES))
    for q in range(STRIPS):
        for a in range(KZ):
            for b in range(5):
                place[q, a, b, KY * a + 2 * q + b] = 1.0
    place = place.reshape(STRIPS * LANES, LANES)
    knots_x = WIDTH // SPACING + 3
    mass_x = np_mass(knots_x, WIDTH)
    full_x = np_basis(np.arange(WIDTH)[None, :], np.arange(knots_x)[:, None]) / mass_x[:, None]
    wide_x = np.zeros((MEMBERS, 8, WIDTH))
    for member in range(MEMBERS):
        wide_x[member, :7] = full_x[4 * member : 4 * member + 7]
    wide_x = wide_x.reshape(MEMBERS * 8, WIDTH)
    gram_x = wide_x @ wide_x.T
    eval_z = np_basis(np.arange(SLABS * DEPTH)[:, None], np.arange(KZ)[None, :])
    eval_y = np_basis(np.arange(STRIPS * ROWS)[:, None], np.arange(KY)[None, :])
    gram_zy = np.zeros((LANES, LANES))
    gram_zy[: KZ * KY, : KZ * KY] = np.kron(eval_z.T @ eval_z, eval_y.T @ eval_y)
    mass_z = np_mass(KZ, SLABS * DEPTH)
    mass_y = np_mass(STACKS * 8 + 3, STACKS * STRIPS * ROWS)
    inverse = np.zeros((STACKS, LANES))
    for stack in range(STACKS):
        inverse[stack, : KZ * KY] = (
            1.0 / (mass_z[:, None] * mass_y[None, 8 * stack : 8 * stack + KY])
        ).reshape(-1)
    ez = eval_z.reshape(SLABS, DEPTH, KZ)
    ey = eval_y.reshape(STRIPS, ROWS, KY)
    lane = np.arange(LANES)
    low = np.where((lane < KZ * KY) & (lane % KY < 3), 1.0, 0.0)
    high = np.where((lane < KZ * KY) & (lane % KY >= 8), 1.0, 0.0)
    ez_l = np.zeros((SLABS, DEPTH, LANES))
    ey_l = np.zeros((STRIPS, ROWS, LANES))
    ez_l[..., : KZ * KY] = np.repeat(ez, KY, axis=2)
    ey_l[..., : KZ * KY] = np.tile(ey, (1, 1, KZ))
    f = lambda v: np.asarray(v, np.float32)
    high_zy = fit_zy.astype(jnp.bfloat16)
    low_zy = (fit_zy - high_zy.astype(np.float32)).astype(jnp.bfloat16)
    fit_zy = np.block([[high_zy, high_zy], [low_zy, np.zeros_like(low_zy)]])
    return dict(
        fit_zy=fit_zy, place=np.asarray(place, jnp.bfloat16), fit_x=f(fit_x), wide_x=f(wide_x), gram_x=f(gram_x), gram_zy=f(gram_zy),
        inverse=f(inverse), ez=f(ez_l), ey=f(ey_l), low=f(low), high=f(high),
    )


def split(x):
    hi = x.astype(BF16)
    return hi, (x - hi.astype(F32)).astype(BF16)


def dot(a, b, dims):
    ah, al = split(a)
    bh, bl = split(b)
    d = lambda u, v: lax.dot_general(u, v, (dims, ((), ())), preferred_element_type=F32)
    return d(ah, bh) + d(ah, bl) + d(al, bh)


NN = ((1,), (0,))
NT = ((1,), (1,))


def pack_kernel(f_ref, m_ref, o_ref, s_ref, b_ref, t_ref, sem):
    copies = [
        pltpu.make_async_copy(ref, b_ref.at[image], sem.at[image])
        for image, ref in enumerate((f_ref, m_ref))
    ]
    for copy in copies:
        copy.start()
    zero = jnp.zeros((RADIUS, LANES), F32)
    for image in range(2):
        s_ref[image, 0:RADIUS, :] = zero
        s_ref[image, RADIUS + WIDTH : 2 * RADIUS + WIDTH, :] = zero
    for image in range(2):
        copies[image].wait()
        for block in range(WIDTH // LANES):
            buf = t_ref.at[image, block]
            buf[...] = b_ref[image, :, block * LANES : (block + 1) * LANES]
            rows = [buf[pl.ds(y, DEPTH, stride=ROWS), :] for y in range(ROWS)]
            tile = jnp.concatenate(rows, axis=0).T
            s_ref[image, RADIUS + block * LANES : RADIUS + (block + 1) * LANES, :] = tile
        for member in range(MEMBERS):
            o_ref[member, image] = s_ref[image, member * COLS : member * COLS + WIDE, :]


def rim_kernel(r_ref, up_ref, down_ref):
    for half in range(2):
        for image in range(2):
            slabs = range(4 * half, 4 * half + 4)
            up_ref[half, image] = jnp.concatenate(
                [r_ref[member_of(g, STRIPS - 1), image, :, 96:128] for g in slabs], axis=1
            )
            down_ref[half, image] = jnp.concatenate(
                [r_ref[member_of(g, 0), image, :, 0:32] for g in slabs], axis=1
            )


def window_x(v):
    roll = pltpu.roll
    s = v + roll(v, WIDE - 1, 0)
    s = s + roll(s, WIDE - 2, 0)
    s = s + roll(s, WIDE - 4, 0)
    return s[0:COLS] + v[2 * RADIUS : 2 * RADIUS + COLS]


def windows(f, m):
    return [window_x(v) for v in (f, m, f * f, m * m, f * m)]


def columns_kernel(r_ref, turned, stack):
    def phase_x(g, carry):
        for q in range(STRIPS):
            i = member_of(g, q)
            values = windows(r_ref[i, 0], r_ref[i, 1])
            values.append(r_ref[i, 0, RADIUS : RADIUS + COLS, :])
            values.append(r_ref[i, 1, RADIUS : RADIUS + COLS, :])
            values.append(
                (
                    r_ref[i, 1, RADIUS + 1 : RADIUS + 1 + COLS, :]
                    - r_ref[i, 1, RADIUS - 1 : RADIUS - 1 + COLS, :]
                )
                * 0.5
            )
            for item, v in enumerate(values):
                stack[item, q * COLS : (q + 1) * COLS, :] = v
        for item in range(8):
            turned[item, g] = stack[item].T
        return carry

    lax.fori_loop(0, SLABS, phase_x, 0)


def force_kernel(
    turned, below_ref, above_ref, fz_ref, fx_ref, place_ref, o_ref, stack, rim_t, summed, mid, fr, acc
):
    roll = pltpu.roll

    for half in range(2):
        for at, ref in ((0, below_ref), (96, above_ref)):
            values = windows(ref[half, 0], ref[half, 1])
            values.append(ref[half, 1, RADIUS : RADIUS + COLS, :])
            for item, v in enumerate(values):
                stack[item, at : at + COLS, :] = v
        for item in range(6):
            stack[item, 32:96, :] = jnp.zeros((64, LANES), F32)
            rim_t[half, item] = stack[item].T

    lane = lax.broadcasted_iota(jnp.int32, (8, LANES), 1)
    first, last = lane < COLS, lane >= LANES - COLS
    row = lambda y: pl.ds(y * 8, 8) if not isinstance(y, int) else slice(y * 8, y * 8 + 8)

    def phase_y(g, carry):
        half = g // 4
        base = (g % 4) * 4
        near = lambda item, i: rim_t[half, item, row(base + i), :]
        for field in range(5):
            v = [turned[field, g, row(y), :] for y in range(ROWS)]
            lower = [jnp.where(first, near(field, i), roll(v[12 + i], COLS, 1)) for i in range(4)]
            upper = [jnp.where(last, near(field, i), roll(v[i], LANES - COLS, 1)) for i in range(4)]
            v = lower + v + upper
            s = [v[i] + v[i + 1] for i in range(23)]
            s = [s[i] + s[i + 2] for i in range(21)]
            for y in range(ROWS):
                summed[field, g, row(y), :] = (s[y] + s[y + 4]) + v[y + 8]
        m0 = turned[6, g, row(0), :]
        m15 = turned[6, g, row(15), :]
        mid[g, row(0), :] = jnp.where(first, near(5, 3), roll(m15, COLS, 1))
        mid[g, row(17), :] = jnp.where(last, near(5, 0), roll(m0, LANES - COLS, 1))
        mid[g, 8 : 8 + LANES, :] = turned[6, g]
        return carry

    lax.fori_loop(0, SLABS, phase_y, 0)

    z = lax.broadcasted_iota(jnp.int32, (8, LANES), 0)
    zero = jnp.zeros((8, LANES), F32)

    def window_z(v):
        v = [zero] + v + [zero]

        def ahead(u, d):
            r = [roll(x, 8 - d, 0) for x in u] + [zero]
            return [x + jnp.where(z < 8 - d, r[i], r[i + 1]) for i, x in enumerate(u)]

        s = ahead(ahead(ahead(v, 1), 2), 4)
        t = [s[i] + v[i + 1] for i in range(SLABS + 1)]
        return [roll(jnp.where(z >= 4, t[g], t[g + 1]), 4, 0) for g in range(SLABS)]

    inv = 1.0 / COUNT

    def phase_z(y, carry):
        sums = [window_z([summed[field, g, row(y), :] for g in range(SLABS)]) for field in range(5)]
        m = [mid[g, row(y + 1), :] for g in range(SLABS)]
        fore = [roll(v, 7, 0) for v in m] + [zero]
        back = [zero] + [roll(v, 1, 0) for v in m]
        for g in range(SLABS):
            grad_z = (
                jnp.where(z < 7, fore[g], fore[g + 1]) - jnp.where(z > 0, back[g + 1], back[g])
            ) * 0.5
            grad_y = (mid[g, row(y + 2), :] - mid[g, row(y), :]) * 0.5
            grad_x = turned[7, g, row(y), :]
            mean_f = sums[0][g] * inv
            mean_m = sums[1][g] * inv
            cov = sums[4][g] * inv - mean_f * mean_m
            var_f = sums[2][g] * inv - mean_f * mean_f
            var_m = sums[3][g] * inv - mean_m * mean_m
            factor = 2.0 * cov / (var_f * var_m + EPS)
            resid = turned[5, g, row(y), :] - mean_f - cov / (var_m + EPS) * (m[g] - mean_m)
            common = factor * resid
            for k, grad in enumerate((grad_z, grad_y, grad_x)):
                fr[g, row(y), k * LANES : (k + 1) * LANES] = common * grad
        return carry

    lax.fori_loop(0, ROWS, phase_z, 0)

    acc[...] = jnp.zeros((16, 8, 3 * LANES), F32)
    for g in range(SLABS):
        hi, lo = split(fr[g])
        part = lax.dot_general(
            fz_ref[...], jnp.concatenate([hi, lo], axis=0), (NN, ((), ())), preferred_element_type=F32
        )
        for a in range(4):
            acc[g + a] += part[8 * a : 8 * a + 8] + part[32 + 8 * a : 40 + 8 * a]
    wide = dot(fx_ref[...], acc[...].reshape(LANES, 3 * LANES), NT)
    wide = jnp.concatenate([wide[24 * q : 24 * q + 24] for q in range(STRIPS)], axis=1)
    mm = lambda u: lax.dot_general(u, place_ref[...], (NN, ((), ())), preferred_element_type=F32)
    hi, lo = split(wide)
    o_ref[...] = mm(hi) + mm(lo)


def fold_kernel(p_ref, below_ref, above_ref, low_ref, high_ref, o_ref):
    total = p_ref[...]
    total += low_ref[...] * pltpu.roll(below_ref[...], LANES - 8, 1)
    total += high_ref[...] * pltpu.roll(above_ref[...], 8, 1)
    for member in range(MEMBERS):
        o_ref[member] = total


def gathered(g_ref, k):
    return jnp.concatenate([g_ref[p, 8 * k : 8 * k + 8, :] for p in range(MEMBERS)], axis=0)


def power_kernel(g_ref, inv_ref, gx_ref, gzy_ref, o_ref):
    inverse = inv_ref[pl.ds(lax.axis_index("xy_0"), 1), :]
    parts = [gathered(g_ref, k) * inverse for k in range(3)]
    mm = lambda u, v: lax.dot_general(u, v, (NN, ((), ())), preferred_element_type=F32)
    halves = [split(part) for part in parts]
    high = jnp.concatenate([h for h, _ in halves], axis=1)
    low = jnp.concatenate([l for _, l in halves], axis=1)
    gh, gl = split(gx_ref[...])
    t = mm(gh, high) + mm(gh, low) + mm(gl, high)
    zh, zl = split(gzy_ref[...])
    zz = jnp.concatenate([zh, zh], axis=0)
    total = jnp.zeros((8, LANES), F32)
    for k, (h, l) in enumerate(halves):
        u = mm(jnp.concatenate([h, l], axis=1), zz) + mm(h, zl)
        product = t[:, k * LANES : (k + 1) * LANES] * u
        total += jnp.sum(product.reshape(MEMBERS, 8, LANES), axis=0)
    total = jnp.full((8, LANES), jnp.sum(total), F32)
    for stack in range(STACKS):
        o_ref[stack] = total


def field_kernel(g_ref, ez_ref, ey_ref, inv_ref, w_ref, o_ref):
    ez = ez_ref[2 * lax.axis_index("gz_0") + lax.axis_index("gz_1")]
    ey = ey_ref[2 * lax.axis_index("xy_1") + lax.axis_index("xy_2")]
    rows = [ez[z : z + 1] * ey for z in range(DEPTH)]
    e = jnp.concatenate(rows, axis=0) * inv_ref[pl.ds(lax.axis_index("xy_0"), 1), :]
    h = dot(e, jnp.concatenate([gathered(g_ref, k) for k in range(3)], axis=0), NT)
    size = 8 * MEMBERS
    h = jnp.concatenate([h[:, k * size : (k + 1) * size] for k in range(3)], axis=0)
    o_ref[...] = dot(h, w_ref[...], NN)


def scale_kernel(size, f_ref, p_ref, o_ref, s_ref, sem):
    power = p_ref[0]
    for stack in range(1, STACKS):
        power = power + p_ref[stack]
    scale = (1.0 / (jnp.sqrt(power / size) + 1e-6))[0:1, 0:1]
    part = 3 * LANES // PARTS
    copies = []
    for i in range(PARTS):
        at = pl.ds(i * part, part)
        s_ref[at] = f_ref[at] * scale
        copies.append(pltpu.make_async_copy(s_ref.at[at], o_ref.at[at], sem.at[i]))
        copies[-1].start()
    for copy in copies:
        copy.wait()


def call(kernel, shapes, *args, scratch=(), flops=0, **kw):
    if flops:
        kw["cost_estimate"] = pl.CostEstimate(flops=flops, transcendentals=0, bytes_accessed=1 << 20)
    return pl.pallas_call(
        kernel,
        out_shape=shapes,
        scratch_shapes=list(scratch),
        compiler_params=pltpu.CompilerParams(vmem_limit_bytes=40 << 20),
        **kw,
    )(*args)


def shards(fixed, moving):
    tab = tables()
    sds = lambda *shape: jax.ShapeDtypeStruct(shape, F32)
    upward = [(i, i + 1) for i in range(STACKS - 1)]
    downward = [(i + 1, i) for i in range(STACKS - 1)]

    flat = (DEPTH * ROWS, WIDTH)
    chunks = call(
        pack_kernel,
        sds(MEMBERS, 2, WIDE, LANES),
        pltpu.with_memory_space_constraint(fixed.reshape(flat), pltpu.HBM),
        pltpu.with_memory_space_constraint(moving.reshape(flat), pltpu.HBM),
        scratch=[
            pltpu.VMEM((2, WIDTH + 2 * RADIUS, LANES), F32),
            pltpu.VMEM((2, LANES, WIDTH), F32),
            pltpu.VMEM((2, WIDTH // LANES, LANES, LANES), F32),
            pltpu.SemaphoreType.DMA((2,)),
        ],
        in_specs=[pl.BlockSpec(memory_space=pltpu.HBM)] * 2,
    )
    blocks = lax.all_to_all(chunks, PLANE, 0, 0)
    up, down = call(rim_kernel, (sds(2, 2, WIDE, LANES), sds(2, 2, WIDE, LANES)), blocks)
    below = lax.ppermute(up, "xy_0", upward)
    above = lax.ppermute(down, "xy_0", downward)
    turned = call(
        columns_kernel,
        sds(8, SLABS, LANES, LANES),
        blocks,
        scratch=[pltpu.VMEM((8, LANES, LANES), F32)],
        flops=1 << 31,
    )
    part = call(
        force_kernel,
        sds(24, LANES),
        turned,
        below,
        above,
        tab["fit_zy"],
        tab["fit_x"],
        tab["place"],
        scratch=[
            pltpu.VMEM((6, LANES, LANES), F32),
            pltpu.VMEM((2, 6, LANES, LANES), F32),
            pltpu.VMEM((5, SLABS, LANES, LANES), F32),
            pltpu.VMEM((SLABS, LANES + 16, LANES), F32),
            pltpu.VMEM((SLABS, LANES, 3 * LANES), F32),
            pltpu.VMEM((16, 8, 3 * LANES), F32),
        ],
    )
    below = lax.ppermute(part, "xy_0", upward)
    above = lax.ppermute(part, "xy_0", downward)
    copies = call(
        fold_kernel,
        sds(MEMBERS, 24, LANES),
        part,
        below,
        above,
        tab["low"][None],
        tab["high"][None],
    )
    numer = lax.all_to_all(copies, PLANE, 0, 0)
    power = call(
        power_kernel, sds(STACKS, 8, LANES), numer, tab["inverse"], tab["gram_x"], tab["gram_zy"]
    )
    powers = lax.all_to_all(power, "xy_0", 0, 0, axis_index_groups=[FROM_MIDDLE])
    size = float(3 * SLABS * DEPTH * STACKS * STRIPS * ROWS * WIDTH)
    field = call(
        field_kernel,
        sds(3 * LANES, WIDTH),
        numer,
        tab["ez"],
        tab["ey"],
        tab["inverse"],
        tab["wide_x"],
        flops=1 << 31,
    )
    field = call(
        functools.partial(scale_kernel, size),
        sds(3 * LANES, WIDTH),
        field,
        powers,
        scratch=[pltpu.VMEM((3 * LANES, WIDTH), F32), pltpu.SemaphoreType.DMA((PARTS,))],
        out_specs=pl.BlockSpec(memory_space=pltpu.HBM),
    )
    return field.reshape(3, DEPTH, ROWS, WIDTH)


def solution(mesh):
    torus = Mesh(mesh.devices.reshape(4, 2, 16, 2, 2), ("gz_0", "gz_1", "xy_0", "xy_1", "xy_2"))
    placed = (P(GZ, XY, None), P(GZ, XY, None))
    return jax.shard_map(
        shards, mesh=torus, in_specs=placed, out_specs=P(None, GZ, XY, None), check_vma=False
    )
```

```python
import functools

import jax
import jax.numpy as jnp
import numpy as np
from jax import lax
from jax.experimental import pallas as pl
from jax.experimental.pallas import tpu as pltpu
from jax.sharding import Mesh
from jax.sharding import PartitionSpec as P


RADIUS = 4
SPACING = 8
EPS = 1e-05
COUNT = float((2 * RADIUS + 1) ** 3)
XY = ("xy_0", "xy_1", "xy_2")
GZ = ("gz_0", "gz_1")
PLANE = ("gz_0", "gz_1", "xy_1", "xy_2")


def member_of(slab, strip):
    place = {"gz_0": slab // 2, "gz_1": slab % 2, "xy_1": strip // 2, "xy_2": strip % 2}
    size = {"gz_0": 4, "gz_1": 2, "xy_1": 2, "xy_2": 2}
    return functools.reduce(lambda total, axis: total * size[axis] + place[axis], PLANE, 0)


SLABS, STRIPS, STACKS = 8, 4, 16
MEMBERS = SLABS * STRIPS
DEPTH, ROWS, WIDTH = 8, 16, 1024
COLS = WIDTH // MEMBERS
FROM_MIDDLE = sorted(range(STACKS), key=lambda i: abs(2 * i - STACKS))
WIDE = COLS + 2 * RADIUS
LANES = 128
KZ = SLABS + 3
KY = STRIPS * ROWS // SPACING + 3
F32 = jnp.float32
BF16 = jnp.bfloat16


def np_basis(index, knot):
    span = index // SPACING
    t = (index - span * SPACING) / SPACING
    j = knot - span
    out = np.where(j == 0, (1 - t) ** 3 / 6, 0.0)
    out = np.where(j == 1, (3 * t**3 - 6 * t**2 + 4) / 6, out)
    out = np.where(j == 2, (-3 * t**3 + 3 * t**2 + 3 * t + 1) / 6, out)
    return np.where(j == 3, t**3 / 6, out)


def np_fit(index, knot):
    value = np_basis(index, knot)
    span = index // SPACING
    total = sum(np_basis(index, span + step) ** 2 for step in range(4))
    return value**3 / total


def np_mass(knots, extent):
    spans = extent // SPACING
    within = np.arange(SPACING)
    energy = [np.sum(np_basis(within, np.full(SPACING, j)) ** 2) for j in range(4)]
    return np.array(
        [sum(energy[j] for j in range(4) if 0 <= c - j <= spans - 1) for c in range(knots)]
    )


def tables():
    z8, y16 = np.arange(DEPTH), np.arange(ROWS)
    fit_z = np_fit(z8[None, :], np.arange(4)[:, None])
    fit_y = np_fit(y16[None, :], np.arange(8)[:, None])
    fit_zy = np.einsum("az,by->abyz", fit_z, fit_y).reshape(32, LANES).astype(np.float32)
    fit_x = np_fit(np.arange(COLS)[None, :], np.arange(8)[:, None])
    fit_x = np.einsum("qr,kj,cx->qkcjrx", np.eye(STRIPS), np.eye(3), fit_x).reshape(96, 3 * LANES)
    place = np.zeros((STRIPS, 16, 8, LANES))
    for q in range(STRIPS):
        for a in range(KZ):
            for b in range(5):
                place[q, a, b, KY * a + 2 * q + b] = 1.0
    place = place.reshape(STRIPS * LANES, LANES)
    knots_x = WIDTH // SPACING + 3
    mass_x = np_mass(knots_x, WIDTH)
    full_x = np_basis(np.arange(WIDTH)[None, :], np.arange(knots_x)[:, None]) / mass_x[:, None]
    wide_x = np.zeros((MEMBERS, 8, WIDTH))
    for member in range(MEMBERS):
        wide_x[member, :7] = full_x[4 * member : 4 * member + 7]
    wide_x = wide_x.reshape(MEMBERS * 8, WIDTH)
    gram_x = wide_x @ wide_x.T
    eval_z = np_basis(np.arange(SLABS * DEPTH)[:, None], np.arange(KZ)[None, :])
    eval_y = np_basis(np.arange(STRIPS * ROWS)[:, None], np.arange(KY)[None, :])
    gram_zy = np.zeros((LANES, LANES))
    gram_zy[: KZ * KY, : KZ * KY] = np.kron(eval_z.T @ eval_z, eval_y.T @ eval_y)
    mass_z = np_mass(KZ, SLABS * DEPTH)
    mass_y = np_mass(STACKS * 8 + 3, STACKS * STRIPS * ROWS)
    inverse = np.zeros((STACKS, LANES))
    for stack in range(STACKS):
        inverse[stack, : KZ * KY] = (
            1.0 / (mass_z[:, None] * mass_y[None, 8 * stack : 8 * stack + KY])
        ).reshape(-1)
    ez = eval_z.reshape(SLABS, DEPTH, KZ)
    ey = eval_y.reshape(STRIPS, ROWS, KY)
    lane = np.arange(LANES)
    low = np.where((lane < KZ * KY) & (lane % KY < 3), 1.0, 0.0)
    high = np.where((lane < KZ * KY) & (lane % KY >= 8), 1.0, 0.0)
    ez_l = np.zeros((SLABS, DEPTH, LANES))
    ey_l = np.zeros((STRIPS, ROWS, LANES))
    ez_l[..., : KZ * KY] = np.repeat(ez, KY, axis=2)
    ey_l[..., : KZ * KY] = np.tile(ey, (1, 1, KZ))
    f = lambda v: np.asarray(v, np.float32)
    high_zy = fit_zy.astype(jnp.bfloat16)
    low_zy = (fit_zy - high_zy.astype(np.float32)).astype(jnp.bfloat16)
    fit_zy = np.block([[high_zy, high_zy], [low_zy, np.zeros_like(low_zy)]])
    return dict(
        fit_zy=fit_zy, place=np.asarray(place, jnp.bfloat16), fit_x=f(fit_x), wide_x=f(wide_x), gram_x=f(gram_x), gram_zy=f(gram_zy),
        inverse=f(inverse), ez=f(ez_l), ey=f(ey_l), low=f(low), high=f(high),
    )


def split(x):
    hi = x.astype(BF16)
    return hi, (x - hi.astype(F32)).astype(BF16)


def dot(a, b, dims):
    ah, al = split(a)
    bh, bl = split(b)
    d = lambda u, v: lax.dot_general(u, v, (dims, ((), ())), preferred_element_type=F32)
    return d(ah, bh) + d(ah, bl) + d(al, bh)


NN = ((1,), (0,))
NT = ((1,), (1,))


def pack_kernel(f_ref, m_ref, o_ref, s_ref, b_ref, t_ref, sem):
    copies = [
        pltpu.make_async_copy(ref, b_ref.at[image], sem.at[image])
        for image, ref in enumerate((f_ref, m_ref))
    ]
    for copy in copies:
        copy.start()
    zero = jnp.zeros((RADIUS, LANES), F32)
    for image in range(2):
        s_ref[image, 0:RADIUS, :] = zero
        s_ref[image, RADIUS + WIDTH : 2 * RADIUS + WIDTH, :] = zero
    for image in range(2):
        copies[image].wait()
        for block in range(WIDTH // LANES):
            buf = t_ref.at[image, block]
            buf[...] = b_ref[image, :, block * LANES : (block + 1) * LANES]
            rows = [buf[pl.ds(y, DEPTH, stride=ROWS), :] for y in range(ROWS)]
            tile = jnp.concatenate(rows, axis=0).T
            s_ref[image, RADIUS + block * LANES : RADIUS + (block + 1) * LANES, :] = tile
        for member in range(MEMBERS):
            o_ref[member, image] = s_ref[image, member * COLS : member * COLS + WIDE, :]


def rim_kernel(r_ref, up_ref, down_ref):
    for half in range(2):
        for image in range(2):
            slabs = range(4 * half, 4 * half + 4)
            up_ref[half, image] = jnp.concatenate(
                [r_ref[member_of(g, STRIPS - 1), image, :, 96:128] for g in slabs], axis=1
            )
            down_ref[half, image] = jnp.concatenate(
                [r_ref[member_of(g, 0), image, :, 0:32] for g in slabs], axis=1
            )


def window_x(v):
    roll = pltpu.roll
    s = v + roll(v, WIDE - 1, 0)
    s = s + roll(s, WIDE - 2, 0)
    s = s + roll(s, WIDE - 4, 0)
    return s[0:COLS] + v[2 * RADIUS : 2 * RADIUS + COLS]


def windows(f, m):
    return [window_x(v) for v in (f, m, f * f, m * m, f * m)]


def columns_kernel(r_ref, turned, stack):
    def phase_x(g, carry):
        for q in range(STRIPS):
            i = member_of(g, q)
            values = windows(r_ref[i, 0], r_ref[i, 1])
            values.append(r_ref[i, 0, RADIUS : RADIUS + COLS, :])
            values.append(r_ref[i, 1, RADIUS : RADIUS + COLS, :])
            values.append(
                (
                    r_ref[i, 1, RADIUS + 1 : RADIUS + 1 + COLS, :]
                    - r_ref[i, 1, RADIUS - 1 : RADIUS - 1 + COLS, :]
                )
                * 0.5
            )
            for item, v in enumerate(values):
                stack[item, q * COLS : (q + 1) * COLS, :] = v
        for item in range(8):
            turned[item, g] = stack[item].T
        return carry

    lax.fori_loop(0, SLABS, phase_x, 0)


def force_kernel(
    turned, below_ref, above_ref, fz_ref, fx_ref, place_ref, o_ref, stack, rim_t, summed, mid, fr, acc
):
    roll = pltpu.roll

    for half in range(2):
        for at, ref in ((0, below_ref), (96, above_ref)):
            values = windows(ref[half, 0], ref[half, 1])
            values.append(ref[half, 1, RADIUS : RADIUS + COLS, :])
            for item, v in enumerate(values):
                stack[item, at : at + COLS, :] = v
        for item in range(6):
            stack[item, 32:96, :] = jnp.zeros((64, LANES), F32)
            rim_t[half, item] = stack[item].T

    lane = lax.broadcasted_iota(jnp.int32, (8, LANES), 1)
    first, last = lane < COLS, lane >= LANES - COLS
    row = lambda y: pl.ds(y * 8, 8) if not isinstance(y, int) else slice(y * 8, y * 8 + 8)

    def phase_y(g, carry):
        half = g // 4
        base = (g % 4) * 4
        near = lambda item, i: rim_t[half, item, row(base + i), :]
        for field in range(5):
            v = [turned[field, g, row(y), :] for y in range(ROWS)]
            lower = [jnp.where(first, near(field, i), roll(v[12 + i], COLS, 1)) for i in range(4)]
            upper = [jnp.where(last, near(field, i), roll(v[i], LANES - COLS, 1)) for i in range(4)]
            v = lower + v + upper
            s = [v[i] + v[i + 1] for i in range(23)]
            s = [s[i] + s[i + 2] for i in range(21)]
            for y in range(ROWS):
                summed[field, g, row(y), :] = (s[y] + s[y + 4]) + v[y + 8]
        m0 = turned[6, g, row(0), :]
        m15 = turned[6, g, row(15), :]
        mid[g, row(0), :] = jnp.where(first, near(5, 3), roll(m15, COLS, 1))
        mid[g, row(17), :] = jnp.where(last, near(5, 0), roll(m0, LANES - COLS, 1))
        mid[g, 8 : 8 + LANES, :] = turned[6, g]
        return carry

    lax.fori_loop(0, SLABS, phase_y, 0)

    z = lax.broadcasted_iota(jnp.int32, (8, LANES), 0)
    zero = jnp.zeros((8, LANES), F32)

    def window_z(v):
        v = [zero] + v + [zero]

        def ahead(u, d):
            r = [roll(x, 8 - d, 0) for x in u] + [zero]
            return [x + jnp.where(z < 8 - d, r[i], r[i + 1]) for i, x in enumerate(u)]

        s = ahead(ahead(ahead(v, 1), 2), 4)
        t = [s[i] + v[i + 1] for i in range(SLABS + 1)]
        return [roll(jnp.where(z >= 4, t[g], t[g + 1]), 4, 0) for g in range(SLABS)]

    inv = 1.0 / COUNT

    def phase_z(y, carry):
        sums = [window_z([summed[field, g, row(y), :] for g in range(SLABS)]) for field in range(5)]
        m = [mid[g, row(y + 1), :] for g in range(SLABS)]
        fore = [roll(v, 7, 0) for v in m] + [zero]
        back = [zero] + [roll(v, 1, 0) for v in m]
        for g in range(SLABS):
            grad_z = (
                jnp.where(z < 7, fore[g], fore[g + 1]) - jnp.where(z > 0, back[g + 1], back[g])
            ) * 0.5
            grad_y = (mid[g, row(y + 2), :] - mid[g, row(y), :]) * 0.5
            grad_x = turned[7, g, row(y), :]
            mean_f = sums[0][g] * inv
            mean_m = sums[1][g] * inv
            cov = sums[4][g] * inv - mean_f * mean_m
            var_f = sums[2][g] * inv - mean_f * mean_f
            var_m = sums[3][g] * inv - mean_m * mean_m
            factor = 2.0 * cov / (var_f * var_m + EPS)
            resid = turned[5, g, row(y), :] - mean_f - cov / (var_m + EPS) * (m[g] - mean_m)
            common = factor * resid
            for k, grad in enumerate((grad_z, grad_y, grad_x)):
                fr[g, row(y), k * LANES : (k + 1) * LANES] = common * grad
        return carry

    lax.fori_loop(0, ROWS, phase_z, 0)

    acc[...] = jnp.zeros((16, 8, 3 * LANES), F32)
    for g in range(SLABS):
        hi, lo = split(fr[g])
        part = lax.dot_general(
            fz_ref[...], jnp.concatenate([hi, lo], axis=0), (NN, ((), ())), preferred_element_type=F32
        )
        for a in range(4):
            acc[g + a] += part[8 * a : 8 * a + 8] + part[32 + 8 * a : 40 + 8 * a]
    wide = dot(fx_ref[...], acc[...].reshape(LANES, 3 * LANES), NT)
    wide = jnp.concatenate([wide[24 * q : 24 * q + 24] for q in range(STRIPS)], axis=1)
    mm = lambda u: lax.dot_general(u, place_ref[...], (NN, ((), ())), preferred_element_type=F32)
    hi, lo = split(wide)
    o_ref[...] = mm(hi) + mm(lo)


def fold_kernel(p_ref, below_ref, above_ref, low_ref, high_ref, o_ref):
    total = p_ref[...]
    total += low_ref[...] * pltpu.roll(below_ref[...], LANES - 8, 1)
    total += high_ref[...] * pltpu.roll(above_ref[...], 8, 1)
    for member in range(MEMBERS):
        o_ref[member] = total


def gathered(g_ref, k):
    return jnp.concatenate([g_ref[p, 8 * k : 8 * k + 8, :] for p in range(MEMBERS)], axis=0)


def power_kernel(g_ref, inv_ref, gx_ref, gzy_ref, o_ref):
    inverse = inv_ref[pl.ds(lax.axis_index("xy_0"), 1), :]
    parts = [gathered(g_ref, k) * inverse for k in range(3)]
    mm = lambda u, v: lax.dot_general(u, v, (NN, ((), ())), preferred_element_type=F32)
    halves = [split(part) for part in parts]
    high = jnp.concatenate([h for h, _ in halves], axis=1)
    low = jnp.concatenate([l for _, l in halves], axis=1)
    gh, gl = split(gx_ref[...])
    t = mm(gh, high) + mm(gh, low) + mm(gl, high)
    zh, zl = split(gzy_ref[...])
    zz = jnp.concatenate([zh, zh], axis=0)
    total = jnp.zeros((8, LANES), F32)
    for k, (h, l) in enumerate(halves):
        u = mm(jnp.concatenate([h, l], axis=1), zz) + mm(h, zl)
        product = t[:, k * LANES : (k + 1) * LANES] * u
        total += jnp.sum(product.reshape(MEMBERS, 8, LANES), axis=0)
    total = jnp.full((8, LANES), jnp.sum(total), F32)
    for stack in range(STACKS):
        o_ref[stack] = total


def field_kernel(size, g_ref, ez_ref, ey_ref, inv_ref, w_ref, p_ref, o_ref, s_ref, sem):
    ez = ez_ref[2 * lax.axis_index("gz_0") + lax.axis_index("gz_1")]
    ey = ey_ref[2 * lax.axis_index("xy_1") + lax.axis_index("xy_2")]
    rows = [ez[z : z + 1] * ey for z in range(DEPTH)]
    e = jnp.concatenate(rows, axis=0) * inv_ref[pl.ds(lax.axis_index("xy_0"), 1), :]
    power = p_ref[0]
    for stack in range(1, STACKS):
        power = power + p_ref[stack]
    e = e * (1.0 / (jnp.sqrt(power / size) + 1e-6))[0:1, 0:1]
    h = dot(e, jnp.concatenate([gathered(g_ref, k) for k in range(3)], axis=0), NT)
    wide = 8 * MEMBERS
    copies = []
    for k in range(3):
        at = pl.ds(k * LANES, LANES)
        s_ref[at] = dot(h[:, k * wide : (k + 1) * wide], w_ref[...], NN)
        copies.append(pltpu.make_async_copy(s_ref.at[at], o_ref.at[at], sem.at[k]))
        copies[-1].start()
    for copy in copies:
        copy.wait()


def call(kernel, shapes, *args, scratch=(), flops=0, **kw):
    if flops:
        kw["cost_estimate"] = pl.CostEstimate(flops=flops, transcendentals=0, bytes_accessed=1 << 20)
    return pl.pallas_call(
        kernel,
        out_shape=shapes,
        scratch_shapes=list(scratch),
        compiler_params=pltpu.CompilerParams(vmem_limit_bytes=40 << 20),
        **kw,
    )(*args)


def body(fixed, moving):
    tab = tables()
    sds = lambda *shape: jax.ShapeDtypeStruct(shape, F32)
    upward = [(i, i + 1) for i in range(STACKS - 1)]
    downward = [(i + 1, i) for i in range(STACKS - 1)]

    flat = (DEPTH * ROWS, WIDTH)
    chunks = call(
        pack_kernel,
        sds(MEMBERS, 2, WIDE, LANES),
        pltpu.with_memory_space_constraint(fixed.reshape(flat), pltpu.HBM),
        pltpu.with_memory_space_constraint(moving.reshape(flat), pltpu.HBM),
        scratch=[
            pltpu.VMEM((2, WIDTH + 2 * RADIUS, LANES), F32),
            pltpu.VMEM((2, LANES, WIDTH), F32),
            pltpu.VMEM((2, WIDTH // LANES, LANES, LANES), F32),
            pltpu.SemaphoreType.DMA((2,)),
        ],
        in_specs=[pl.BlockSpec(memory_space=pltpu.HBM)] * 2,
    )
    blocks = lax.all_to_all(chunks, PLANE, 0, 0)
    up, down = call(rim_kernel, (sds(2, 2, WIDE, LANES), sds(2, 2, WIDE, LANES)), blocks)
    below = lax.ppermute(up, "xy_0", upward)
    above = lax.ppermute(down, "xy_0", downward)
    turned = call(
        columns_kernel,
        sds(8, SLABS, LANES, LANES),
        blocks,
        scratch=[pltpu.VMEM((8, LANES, LANES), F32)],
        flops=1 << 31,
    )
    part = call(
        force_kernel,
        sds(24, LANES),
        turned,
        below,
        above,
        tab["fit_zy"],
        tab["fit_x"],
        tab["place"],
        scratch=[
            pltpu.VMEM((6, LANES, LANES), F32),
            pltpu.VMEM((2, 6, LANES, LANES), F32),
            pltpu.VMEM((5, SLABS, LANES, LANES), F32),
            pltpu.VMEM((SLABS, LANES + 16, LANES), F32),
            pltpu.VMEM((SLABS, LANES, 3 * LANES), F32),
            pltpu.VMEM((16, 8, 3 * LANES), F32),
        ],
    )
    below = lax.ppermute(part, "xy_0", upward)
    above = lax.ppermute(part, "xy_0", downward)
    copies = call(
        fold_kernel,
        sds(MEMBERS, 24, LANES),
        part,
        below,
        above,
        tab["low"][None],
        tab["high"][None],
    )
    numer = lax.all_to_all(copies, PLANE, 0, 0)
    power = call(
        power_kernel, sds(STACKS, 8, LANES), numer, tab["inverse"], tab["gram_x"], tab["gram_zy"]
    )
    powers = lax.all_to_all(power, "xy_0", 0, 0, axis_index_groups=[FROM_MIDDLE])
    size = float(3 * SLABS * DEPTH * STACKS * STRIPS * ROWS * WIDTH)
    field = call(
        functools.partial(field_kernel, size),
        sds(3 * LANES, WIDTH),
        numer,
        tab["ez"],
        tab["ey"],
        tab["inverse"],
        tab["wide_x"],
        powers,
        scratch=[pltpu.VMEM((3 * LANES, WIDTH), F32), pltpu.SemaphoreType.DMA((3,))],
        out_specs=pl.BlockSpec(memory_space=pltpu.HBM),
    )
    return field.reshape(3, DEPTH, ROWS, WIDTH)


def solution(mesh):
    torus = Mesh(mesh.devices.reshape(4, 2, 16, 2, 2), ("gz_0", "gz_1", "xy_0", "xy_1", "xy_2"))
    placed = (P(GZ, XY, None), P(GZ, XY, None))
    return jax.shard_map(
        body, mesh=torus, in_specs=placed, out_specs=P(None, GZ, XY, None), check_vma=False
    )
```

```python
import functools

import jax
import jax.numpy as jnp
import numpy as np
from jax import lax
from jax.experimental import pallas as pl
from jax.experimental.pallas import tpu as pltpu
from jax.sharding import Mesh
from jax.sharding import PartitionSpec as P


RADIUS = 4
SPACING = 8
EPS = 1e-05
COUNT = float((2 * RADIUS + 1) ** 3)
XY = ("xy_0", "xy_1", "xy_2")
GZ = ("gz_0", "gz_1")
PLANE = ("gz_0", "gz_1", "xy_1", "xy_2")


def member_of(slab, strip):
    place = {"gz_0": slab // 2, "gz_1": slab % 2, "xy_1": strip // 2, "xy_2": strip % 2}
    size = {"gz_0": 4, "gz_1": 2, "xy_1": 2, "xy_2": 2}
    return functools.reduce(lambda total, axis: total * size[axis] + place[axis], PLANE, 0)


SLABS, STRIPS, STACKS = 8, 4, 16
MEMBERS = SLABS * STRIPS
DEPTH, ROWS, WIDTH = 8, 16, 1024
COLS = WIDTH // MEMBERS
FROM_MIDDLE = sorted(range(STACKS), key=lambda i: abs(2 * i - STACKS))
WIDE = COLS + 2 * RADIUS
LANES = 128
PARTS = 6
KZ = SLABS + 3
KY = STRIPS * ROWS // SPACING + 3
F32 = jnp.float32
BF16 = jnp.bfloat16


def np_basis(index, knot):
    span = index // SPACING
    t = (index - span * SPACING) / SPACING
    j = knot - span
    out = np.where(j == 0, (1 - t) ** 3 / 6, 0.0)
    out = np.where(j == 1, (3 * t**3 - 6 * t**2 + 4) / 6, out)
    out = np.where(j == 2, (-3 * t**3 + 3 * t**2 + 3 * t + 1) / 6, out)
    return np.where(j == 3, t**3 / 6, out)


def np_fit(index, knot):
    value = np_basis(index, knot)
    span = index // SPACING
    total = sum(np_basis(index, span + step) ** 2 for step in range(4))
    return value**3 / total


def np_mass(knots, extent):
    spans = extent // SPACING
    within = np.arange(SPACING)
    energy = [np.sum(np_basis(within, np.full(SPACING, j)) ** 2) for j in range(4)]
    return np.array(
        [sum(energy[j] for j in range(4) if 0 <= c - j <= spans - 1) for c in range(knots)]
    )


def tables():
    z8, y16 = np.arange(DEPTH), np.arange(ROWS)
    fit_z = np_fit(z8[None, :], np.arange(4)[:, None])
    fit_y = np_fit(y16[None, :], np.arange(8)[:, None])
    fit_zy = np.einsum("az,by->abyz", fit_z, fit_y).reshape(32, LANES).astype(np.float32)
    fit_x = np_fit(np.arange(COLS)[None, :], np.arange(8)[:, None])
    fit_x = np.einsum("qr,kj,cx->qkcjrx", np.eye(STRIPS), np.eye(3), fit_x).reshape(96, 3 * LANES)
    place = np.zeros((STRIPS, 16, 8, LANES))
    for q in range(STRIPS):
        for a in range(KZ):
            for b in range(5):
                place[q, a, b, KY * a + 2 * q + b] = 1.0
    place = place.reshape(STRIPS * LANES, LANES)
    knots_x = WIDTH // SPACING + 3
    mass_x = np_mass(knots_x, WIDTH)
    full_x = np_basis(np.arange(WIDTH)[None, :], np.arange(knots_x)[:, None]) / mass_x[:, None]
    wide_x = np.zeros((MEMBERS, 8, WIDTH))
    for member in range(MEMBERS):
        wide_x[member, :7] = full_x[4 * member : 4 * member + 7]
    wide_x = wide_x.reshape(MEMBERS * 8, WIDTH)
    gram_x = wide_x @ wide_x.T
    eval_z = np_basis(np.arange(SLABS * DEPTH)[:, None], np.arange(KZ)[None, :])
    eval_y = np_basis(np.arange(STRIPS * ROWS)[:, None], np.arange(KY)[None, :])
    gram_zy = np.zeros((LANES, LANES))
    gram_zy[: KZ * KY, : KZ * KY] = np.kron(eval_z.T @ eval_z, eval_y.T @ eval_y)
    mass_z = np_mass(KZ, SLABS * DEPTH)
    mass_y = np_mass(STACKS * 8 + 3, STACKS * STRIPS * ROWS)
    inverse = np.zeros((STACKS, LANES))
    for stack in range(STACKS):
        inverse[stack, : KZ * KY] = (
            1.0 / (mass_z[:, None] * mass_y[None, 8 * stack : 8 * stack + KY])
        ).reshape(-1)
    ez = eval_z.reshape(SLABS, DEPTH, KZ)
    ey = eval_y.reshape(STRIPS, ROWS, KY)
    lane = np.arange(LANES)
    low = np.where((lane < KZ * KY) & (lane % KY < 3), 1.0, 0.0)
    high = np.where((lane < KZ * KY) & (lane % KY >= 8), 1.0, 0.0)
    ez_l = np.zeros((SLABS, DEPTH, LANES))
    ey_l = np.zeros((STRIPS, ROWS, LANES))
    ez_l[..., : KZ * KY] = np.repeat(ez, KY, axis=2)
    ey_l[..., : KZ * KY] = np.tile(ey, (1, 1, KZ))
    f = lambda v: np.asarray(v, np.float32)

    def pair(v):
        high = f(v).astype(jnp.bfloat16)
        return np.stack([high, (f(v) - high.astype(np.float32)).astype(jnp.bfloat16)])

    high_zy = fit_zy.astype(jnp.bfloat16)
    low_zy = (fit_zy - high_zy.astype(np.float32)).astype(jnp.bfloat16)
    fit_zy = np.block([[high_zy, high_zy], [low_zy, np.zeros_like(low_zy)]])
    return dict(
        fit_zy=fit_zy, place=np.asarray(place, jnp.bfloat16), fit_x=f(fit_x), wide_x=pair(wide_x), gram_x=pair(gram_x), gram_zy=pair(gram_zy),
        inverse=f(inverse), ez=f(ez_l), ey=f(ey_l), low=f(low), high=f(high),
    )


def split(x):
    hi = x.astype(BF16)
    return hi, (x - hi.astype(F32)).astype(BF16)


def dot(a, b, dims):
    ah, al = split(a)
    bh, bl = split(b)
    d = lambda u, v: lax.dot_general(u, v, (dims, ((), ())), preferred_element_type=F32)
    return d(ah, bh) + d(ah, bl) + d(al, bh)


NN = ((1,), (0,))
NT = ((1,), (1,))


def pack_kernel(f_ref, m_ref, o_ref, s_ref, b_ref, t_ref, sem):
    copies = [
        pltpu.make_async_copy(ref, b_ref.at[image], sem.at[image])
        for image, ref in enumerate((f_ref, m_ref))
    ]
    for copy in copies:
        copy.start()
    zero = jnp.zeros((RADIUS, LANES), F32)
    for image in range(2):
        s_ref[image, 0:RADIUS, :] = zero
        s_ref[image, RADIUS + WIDTH : 2 * RADIUS + WIDTH, :] = zero
    for image in range(2):
        copies[image].wait()
        for block in range(WIDTH // LANES):
            buf = t_ref.at[image, block]
            buf[...] = b_ref[image, :, block * LANES : (block + 1) * LANES]
            rows = [buf[pl.ds(y, DEPTH, stride=ROWS), :] for y in range(ROWS)]
            tile = jnp.concatenate(rows, axis=0).T
            s_ref[image, RADIUS + block * LANES : RADIUS + (block + 1) * LANES, :] = tile
        for member in range(MEMBERS):
            o_ref[member, image] = s_ref[image, member * COLS : member * COLS + WIDE, :]


def rim_kernel(r_ref, up_ref, down_ref):
    for half in range(2):
        for image in range(2):
            slabs = range(4 * half, 4 * half + 4)
            up_ref[half, image] = jnp.concatenate(
                [r_ref[member_of(g, STRIPS - 1), image, :, 96:128] for g in slabs], axis=1
            )
            down_ref[half, image] = jnp.concatenate(
                [r_ref[member_of(g, 0), image, :, 0:32] for g in slabs], axis=1
            )


def window_x(v):
    roll = pltpu.roll
    s = v + roll(v, WIDE - 1, 0)
    s = s + roll(s, WIDE - 2, 0)
    s = s + roll(s, WIDE - 4, 0)
    return s[0:COLS] + v[2 * RADIUS : 2 * RADIUS + COLS]


def windows(f, m):
    return [window_x(v) for v in (f, m, f * f, m * m, f * m)]


def columns_kernel(r_ref, turned, stack):
    def phase_x(g, carry):
        for q in range(STRIPS):
            i = member_of(g, q)
            values = windows(r_ref[i, 0], r_ref[i, 1])
            values.append(r_ref[i, 0, RADIUS : RADIUS + COLS, :])
            values.append(r_ref[i, 1, RADIUS : RADIUS + COLS, :])
            values.append(
                (
                    r_ref[i, 1, RADIUS + 1 : RADIUS + 1 + COLS, :]
                    - r_ref[i, 1, RADIUS - 1 : RADIUS - 1 + COLS, :]
                )
                * 0.5
            )
            for item, v in enumerate(values):
                stack[item, q * COLS : (q + 1) * COLS, :] = v
        for item in range(8):
            turned[item, g] = stack[item].T
        return carry

    lax.fori_loop(0, SLABS, phase_x, 0)


def force_kernel(
    turned, below_ref, above_ref, fz_ref, fx_ref, place_ref, o_ref, stack, rim_t, summed, mid, fr, acc
):
    roll = pltpu.roll

    for half in range(2):
        for at, ref in ((0, below_ref), (96, above_ref)):
            values = windows(ref[half, 0], ref[half, 1])
            values.append(ref[half, 1, RADIUS : RADIUS + COLS, :])
            for item, v in enumerate(values):
                stack[item, at : at + COLS, :] = v
        for item in range(6):
            stack[item, 32:96, :] = jnp.zeros((64, LANES), F32)
            rim_t[half, item] = stack[item].T

    lane = lax.broadcasted_iota(jnp.int32, (8, LANES), 1)
    first, last = lane < COLS, lane >= LANES - COLS
    row = lambda y: pl.ds(y * 8, 8) if not isinstance(y, int) else slice(y * 8, y * 8 + 8)

    def phase_y(g, carry):
        half = g // 4
        base = (g % 4) * 4
        near = lambda item, i: rim_t[half, item, row(base + i), :]
        for field in range(5):
            v = [turned[field, g, row(y), :] for y in range(ROWS)]
            lower = [jnp.where(first, near(field, i), roll(v[12 + i], COLS, 1)) for i in range(4)]
            upper = [jnp.where(last, near(field, i), roll(v[i], LANES - COLS, 1)) for i in range(4)]
            v = lower + v + upper
            s = [v[i] + v[i + 1] for i in range(23)]
            s = [s[i] + s[i + 2] for i in range(21)]
            for y in range(ROWS):
                summed[field, g, row(y), :] = (s[y] + s[y + 4]) + v[y + 8]
        m0 = turned[6, g, row(0), :]
        m15 = turned[6, g, row(15), :]
        mid[g, row(0), :] = jnp.where(first, near(5, 3), roll(m15, COLS, 1))
        mid[g, row(17), :] = jnp.where(last, near(5, 0), roll(m0, LANES - COLS, 1))
        mid[g, 8 : 8 + LANES, :] = turned[6, g]
        return carry

    lax.fori_loop(0, SLABS, phase_y, 0)

    z = lax.broadcasted_iota(jnp.int32, (8, LANES), 0)
    zero = jnp.zeros((8, LANES), F32)

    def window_z(v):
        v = [zero] + v + [zero]

        def ahead(u, d):
            r = [roll(x, 8 - d, 0) for x in u] + [zero]
            return [x + jnp.where(z < 8 - d, r[i], r[i + 1]) for i, x in enumerate(u)]

        s = ahead(ahead(ahead(v, 1), 2), 4)
        t = [s[i] + v[i + 1] for i in range(SLABS + 1)]
        return [roll(jnp.where(z >= 4, t[g], t[g + 1]), 4, 0) for g in range(SLABS)]

    inv = 1.0 / COUNT

    def phase_z(y, carry):
        sums = [window_z([summed[field, g, row(y), :] for g in range(SLABS)]) for field in range(5)]
        m = [mid[g, row(y + 1), :] for g in range(SLABS)]
        fore = [roll(v, 7, 0) for v in m] + [zero]
        back = [zero] + [roll(v, 1, 0) for v in m]
        for g in range(SLABS):
            grad_z = (
                jnp.where(z < 7, fore[g], fore[g + 1]) - jnp.where(z > 0, back[g + 1], back[g])
            ) * 0.5
            grad_y = (mid[g, row(y + 2), :] - mid[g, row(y), :]) * 0.5
            grad_x = turned[7, g, row(y), :]
            mean_f = sums[0][g] * inv
            mean_m = sums[1][g] * inv
            cov = sums[4][g] * inv - mean_f * mean_m
            var_f = sums[2][g] * inv - mean_f * mean_f
            var_m = sums[3][g] * inv - mean_m * mean_m
            factor = 2.0 * cov / (var_f * var_m + EPS)
            resid = turned[5, g, row(y), :] - mean_f - cov / (var_m + EPS) * (m[g] - mean_m)
            common = factor * resid
            for k, grad in enumerate((grad_z, grad_y, grad_x)):
                fr[g, row(y), k * LANES : (k + 1) * LANES] = common * grad
        return carry

    lax.fori_loop(0, ROWS, phase_z, 0)

    acc[...] = jnp.zeros((16, 8, 3 * LANES), F32)
    for g in range(SLABS):
        hi, lo = split(fr[g])
        part = lax.dot_general(
            fz_ref[...], jnp.concatenate([hi, lo], axis=0), (NN, ((), ())), preferred_element_type=F32
        )
        for a in range(4):
            acc[g + a] += part[8 * a : 8 * a + 8] + part[32 + 8 * a : 40 + 8 * a]
    wide = dot(fx_ref[...], acc[...].reshape(LANES, 3 * LANES), NT)
    wide = jnp.concatenate([wide[24 * q : 24 * q + 24] for q in range(STRIPS)], axis=1)
    mm = lambda u: lax.dot_general(u, place_ref[...], (NN, ((), ())), preferred_element_type=F32)
    hi, lo = split(wide)
    o_ref[...] = mm(hi) + mm(lo)


def fold_kernel(p_ref, below_ref, above_ref, low_ref, high_ref, o_ref):
    total = p_ref[...]
    total += low_ref[...] * pltpu.roll(below_ref[...], LANES - 8, 1)
    total += high_ref[...] * pltpu.roll(above_ref[...], 8, 1)
    for member in range(MEMBERS):
        o_ref[member] = total


def gathered(g_ref, k):
    return jnp.concatenate([g_ref[p, 8 * k : 8 * k + 8, :] for p in range(MEMBERS)], axis=0)


def power_kernel(g_ref, inv_ref, gx_ref, gzy_ref, o_ref):
    inverse = inv_ref[pl.ds(lax.axis_index("xy_0"), 1), :]
    parts = [gathered(g_ref, k) * inverse for k in range(3)]
    mm = lambda u, v: lax.dot_general(u, v, (NN, ((), ())), preferred_element_type=F32)
    halves = [split(part) for part in parts]
    high = jnp.concatenate([h for h, _ in halves], axis=1)
    low = jnp.concatenate([l for _, l in halves], axis=1)
    gh, gl = gx_ref[0], gx_ref[1]
    t = mm(gh, high) + mm(gh, low) + mm(gl, high)
    zh, zl = gzy_ref[0], gzy_ref[1]
    zz = jnp.concatenate([zh, zh], axis=0)
    total = jnp.zeros((8, LANES), F32)
    for k, (h, l) in enumerate(halves):
        u = mm(jnp.concatenate([h, l], axis=1), zz) + mm(h, zl)
        product = t[:, k * LANES : (k + 1) * LANES] * u
        total += jnp.sum(product.reshape(MEMBERS, 8, LANES), axis=0)
    total = jnp.full((8, LANES), jnp.sum(total), F32)
    for stack in range(STACKS):
        o_ref[stack] = total


def field_kernel(g_ref, ez_ref, ey_ref, inv_ref, w_ref, o_ref):
    ez = ez_ref[2 * lax.axis_index("gz_0") + lax.axis_index("gz_1")]
    ey = ey_ref[2 * lax.axis_index("xy_1") + lax.axis_index("xy_2")]
    rows = [ez[z : z + 1] * ey for z in range(DEPTH)]
    e = jnp.concatenate(rows, axis=0) * inv_ref[pl.ds(lax.axis_index("xy_0"), 1), :]
    h = dot(e, jnp.concatenate([gathered(g_ref, k) for k in range(3)], axis=0), NT)
    size = 8 * MEMBERS
    h = jnp.concatenate([h[:, k * size : (k + 1) * size] for k in range(3)], axis=0)
    hi, lo = split(h)
    mm = lambda u, v: lax.dot_general(u, v, (NN, ((), ())), preferred_element_type=F32)
    o_ref[...] = mm(hi, w_ref[0]) + mm(hi, w_ref[1]) + mm(lo, w_ref[0])


def scale_kernel(size, f_ref, p_ref, o_ref, s_ref, sem):
    power = p_ref[0]
    for stack in range(1, STACKS):
        power = power + p_ref[stack]
    scale = (1.0 / (jnp.sqrt(power / size) + 1e-6))[0:1, 0:1]
    part = 3 * LANES // PARTS
    copies = []
    for i in range(PARTS):
        at = pl.ds(i * part, part)
        s_ref[at] = f_ref[at] * scale
        copies.append(pltpu.make_async_copy(s_ref.at[at], o_ref.at[at], sem.at[i]))
        copies[-1].start()
    for copy in copies:
        copy.wait()


def call(kernel, shapes, *args, scratch=(), flops=0, **kw):
    if flops:
        kw["cost_estimate"] = pl.CostEstimate(flops=flops, transcendentals=0, bytes_accessed=1 << 20)
    return pl.pallas_call(
        kernel,
        out_shape=shapes,
        scratch_shapes=list(scratch),
        compiler_params=pltpu.CompilerParams(vmem_limit_bytes=40 << 20),
        **kw,
    )(*args)


def body(fixed, moving):
    tab = tables()
    sds = lambda *shape: jax.ShapeDtypeStruct(shape, F32)
    upward = [(i, i + 1) for i in range(STACKS - 1)]
    downward = [(i + 1, i) for i in range(STACKS - 1)]

    flat = (DEPTH * ROWS, WIDTH)
    chunks = call(
        pack_kernel,
        sds(MEMBERS, 2, WIDE, LANES),
        pltpu.with_memory_space_constraint(fixed.reshape(flat), pltpu.HBM),
        pltpu.with_memory_space_constraint(moving.reshape(flat), pltpu.HBM),
        scratch=[
            pltpu.VMEM((2, WIDTH + 2 * RADIUS, LANES), F32),
            pltpu.VMEM((2, LANES, WIDTH), F32),
            pltpu.VMEM((2, WIDTH // LANES, LANES, LANES), F32),
            pltpu.SemaphoreType.DMA((2,)),
        ],
        in_specs=[pl.BlockSpec(memory_space=pltpu.HBM)] * 2,
    )
    blocks = lax.all_to_all(chunks, PLANE, 0, 0)
    up, down = call(rim_kernel, (sds(2, 2, WIDE, LANES), sds(2, 2, WIDE, LANES)), blocks)
    below = lax.ppermute(up, "xy_0", upward)
    above = lax.ppermute(down, "xy_0", downward)
    turned = call(
        columns_kernel,
        sds(8, SLABS, LANES, LANES),
        blocks,
        scratch=[pltpu.VMEM((8, LANES, LANES), F32)],
        flops=1 << 31,
    )
    part = call(
        force_kernel,
        sds(24, LANES),
        turned,
        below,
        above,
        tab["fit_zy"],
        tab["fit_x"],
        tab["place"],
        scratch=[
            pltpu.VMEM((6, LANES, LANES), F32),
            pltpu.VMEM((2, 6, LANES, LANES), F32),
            pltpu.VMEM((5, SLABS, LANES, LANES), F32),
            pltpu.VMEM((SLABS, LANES + 16, LANES), F32),
            pltpu.VMEM((SLABS, LANES, 3 * LANES), F32),
            pltpu.VMEM((16, 8, 3 * LANES), F32),
        ],
    )
    below = lax.ppermute(part, "xy_0", upward)
    above = lax.ppermute(part, "xy_0", downward)
    copies = call(
        fold_kernel,
        sds(MEMBERS, 24, LANES),
        part,
        below,
        above,
        tab["low"][None],
        tab["high"][None],
    )
    numer = lax.all_to_all(copies, PLANE, 0, 0)
    power = call(
        power_kernel, sds(STACKS, 8, LANES), numer, tab["inverse"], tab["gram_x"], tab["gram_zy"]
    )
    powers = lax.all_to_all(power, "xy_0", 0, 0, axis_index_groups=[FROM_MIDDLE])
    size = float(3 * SLABS * DEPTH * STACKS * STRIPS * ROWS * WIDTH)
    field = call(
        field_kernel,
        sds(3 * LANES, WIDTH),
        numer,
        tab["ez"],
        tab["ey"],
        tab["inverse"],
        tab["wide_x"],
        flops=1 << 31,
    )
    field = call(
        functools.partial(scale_kernel, size),
        sds(3 * LANES, WIDTH),
        field,
        powers,
        scratch=[pltpu.VMEM((3 * LANES, WIDTH), F32), pltpu.SemaphoreType.DMA((PARTS,))],
        out_specs=pl.BlockSpec(memory_space=pltpu.HBM),
    )
    return field.reshape(3, DEPTH, ROWS, WIDTH)


def solution(mesh):
    torus = Mesh(mesh.devices.reshape(4, 2, 16, 2, 2), ("gz_0", "gz_1", "xy_0", "xy_1", "xy_2"))
    placed = (P(GZ, XY, None), P(GZ, XY, None))
    return jax.shard_map(
        body, mesh=torus, in_specs=placed, out_specs=P(None, GZ, XY, None), check_vma=False
    )
```
